32 devices in a mesh: fsdp: 4 (over z), width: 4 (over y, x), trial: 2 (over core).
Axes of the slice: x: 2, y: 2, z: 4, core: 2. Of those that a mesh axis runs over, the one named last changes fastest.
Arguments:
- weight_query: bfloat16 [7168, 4096], P(('trial', 'fsdp'), 'width'), parts along dimension 0, may hold values from -0.125 to 0.125
- low_query: bfloat16 [7168, 16], P(('trial', 'fsdp')), parts along dimension 0, may hold values from -0.09375 to 0.09375
- high_query: bfloat16 [32, 4096], P('trial', 'width'), parts along dimension 0, may hold values from -1.5 to 1.5
- weight_key: bfloat16 [7168, 2048], P(('trial', 'fsdp'), 'width'), parts along dimension 0, may hold values from -0.125 to 0.125
- low_key: bfloat16 [7168, 16], P(('trial', 'fsdp')), parts along dimension 0, may hold values from -0.09375 to 0.09375
- high_key: bfloat16 [32, 2048], P('trial', 'width'), parts along dimension 0, may hold values from -1.5 to 1.5
- weight_value: bfloat16 [7168, 2048], P(('trial', 'fsdp'), 'width'), parts along dimension 0, may hold values from -0.125 to 0.125
- low_value: bfloat16 [7168, 16], P(('trial', 'fsdp')), parts along dimension 0, may hold values from -0.09375 to 0.09375
- high_value: bfloat16 [32, 2048], P('trial', 'width'), parts along dimension 0, may hold values from -1.5 to 1.5
- norm_train: float32 [7168], P(('trial', 'fsdp', 'width')), parts along dimension 0, may hold values from 0.25 to 1.75
- norm_step: float32 [7168], P(('trial', 'fsdp', 'width')), parts along dimension 0, may hold values from -0.3 to 0.3
Outputs:
- final_query: bfloat16 [7168, 4096], P('trial', 'width'), parts along dimension 0
- final_key: bfloat16 [7168, 2048], P('trial', 'width'), parts along dimension 0
- final_value: bfloat16 [7168, 2048], P('trial', 'width'), parts along dimension 0
- column_query: float32 [8192], P(('trial', 'width')), parts along dimension 0
- column_key: float32 [4096], P(('trial', 'width')), parts along dimension 0
- column_value: float32 [4096], P(('trial', 'width')), parts along dimension 0
- serve_norm: bfloat16 [7168], P('trial'), parts along dimension 0
The draws below stay inside these ranges and needn't reach their ends.
There are 2 independent parts, one for each index of `trial`. The reference program is written for one: setup_inputs(seed, part) draws one part's arguments, and reference() takes and returns one part's arrays. A program takes and returns all parts, laid end to end along the dimension named above; each array names one. Nothing has to cross between parts.
All inputs are finite; a program needn't handle non-finite values. Where the reference program divides by a largest or mean magnitude, that divisor is 1e-20 or more.
Results may differ from the reference program's by a relative error of at most 0.001.
Values may be sent and summed in bfloat16 or wider, within the bound.
A program may use at most 64 MiB of HBM per device.

```python
import jax
import jax.numpy as jnp

D_MODEL = 3584
Q_DIM = 4096
KV_DIM = 2048
RANK = 16


def strengthened(result, key, source, target, shards_of, factor):
    owner, partner = [(jnp.arange(result.shape[position]) // (result.shape[position] // shards_of)).reshape([-1 if axis == position else 1 for axis in range(result.ndim)]) for position in (source, target)]
    chosen = jax.random.permutation(key, shards_of)[partner]
    strong = (owner == chosen) | (owner == (partner + shards_of // 2) % shards_of)
    return jnp.where(strong, factor * result, result)


def block_levels(key, shape, cuts, least, largest):
    gain, own = 1.0, jax.random.fold_in(key, 6)
    for position, shards_of in cuts:
        draws = jnp.exp(jax.random.uniform(jax.random.fold_in(own, position), (shards_of,), jnp.float32, least / len(cuts), largest / len(cuts)))
        gain = gain * jnp.repeat(draws, shape[position] // shards_of).reshape([-1 if axis == position else 1 for axis in range(len(shape))])
    return gain


def normal_values(own_key, extent, deviation, reach, cuts=(), dtype=jnp.bfloat16):
    drawn = jax.random.normal(own_key, extent, jnp.float32) * deviation
    if len(cuts) > 0:
        drawn = block_levels(own_key, extent, cuts, -0.22, 0.18) * drawn
    return jnp.clip(drawn, min=-reach, max=reach).astype(dtype)


def heavy_noise(rng, shape, scale, bound, pieces, heavy, held_as=jnp.bfloat16):
    entries = scale * jax.random.normal(rng, shape, jnp.float32)
    if pieces:
        entries = entries * block_levels(rng, shape, pieces, -0.22, 0.18)
    return jnp.clip(strengthened(entries, jax.random.fold_in(rng, 3), *heavy), -bound, bound).astype(held_as)


def setup_inputs(seed: int = 0, part: int = 0) -> dict:
    key_of = jax.random.split(jax.random.key(seed), 12)
    own_keys = jax.random.split(jax.random.fold_in(key_of[11], part), 12)
    return {
        "weight_query": heavy_noise(own_keys[0], (D_MODEL, Q_DIM), D_MODEL ** -0.5, 0.125, ((0, 4), (1, 4)), (0, 1, 4, 2.0)),
        "low_query": normal_values(own_keys[1], (D_MODEL, RANK), D_MODEL ** -0.5, 0.09375, ((0, 4),)),
        "high_query": normal_values(own_keys[2], (RANK, Q_DIM), RANK ** -0.5, 1.5, ((1, 4),)),
        "weight_key": heavy_noise(own_keys[3], (D_MODEL, KV_DIM), D_MODEL ** -0.5, 0.125, ((0, 4), (1, 4)), (0, 1, 4, 2.0)),
        "low_key": normal_values(own_keys[4], (D_MODEL, RANK), D_MODEL ** -0.5, 0.09375, ((0, 4),)),
        "high_key": normal_values(own_keys[5], (RANK, KV_DIM), RANK ** -0.5, 1.5, ((1, 4),)),
        "weight_value": heavy_noise(own_keys[6], (D_MODEL, KV_DIM), D_MODEL ** -0.5, 0.125, ((0, 4), (1, 4)), (0, 1, 4, 2.0)),
        "low_value": normal_values(own_keys[7], (D_MODEL, RANK), D_MODEL ** -0.5, 0.09375, ((0, 4),)),
        "high_value": normal_values(own_keys[8], (RANK, KV_DIM), RANK ** -0.5, 1.5, ((1, 4),)),
        "norm_train": jnp.clip(1.0 + 0.15 * jax.random.normal(own_keys[9], (D_MODEL,), jnp.float32), 0.25, 1.75),
        "norm_step": jnp.clip(jax.random.uniform(own_keys[10], (D_MODEL,), jnp.float32, -0.3, 0.3) * block_levels(own_keys[10], (D_MODEL,), ((0, 16),), -0.4, 0.0), -0.3, 0.3),
    }


mix_rate = 2.0


def reference(weight_query, low_query, high_query, weight_key, low_key, high_key, weight_value, low_value, high_value, norm_train, norm_step):
    result_query = weight_query.astype(jnp.float32) + mix_rate * jnp.dot(low_query, high_query, preferred_element_type=jnp.float32)
    result_key = weight_key.astype(jnp.float32) + mix_rate * jnp.dot(low_key, high_key, preferred_element_type=jnp.float32)
    result_value = weight_value.astype(jnp.float32) + mix_rate * jnp.dot(low_value, high_value, preferred_element_type=jnp.float32)
    column_query = jnp.max(jnp.abs(result_query), axis=0)
    final_query = (result_query / column_query).astype(jnp.bfloat16)
    column_key = jnp.max(jnp.abs(result_key), axis=0)
    final_key = (result_key / column_key).astype(jnp.bfloat16)
    column_value = jnp.max(jnp.abs(result_value), axis=0)
    final_value = (result_value / column_value).astype(jnp.bfloat16)
    serve_norm = (norm_train + norm_step).astype(jnp.bfloat16)
    return final_query, final_key, final_value, column_query, column_key, column_value, serve_norm
```

```python
import functools

import jax
import jax.numpy as jnp
from jax import lax
from jax.experimental import pallas as pl
from jax.experimental.pallas import tpu as pltpu
from jax.sharding import PartitionSpec as P

mix_rate = 2.0
MESH = pl.DeviceIdType.MESH
F32, BF16 = jnp.float32, jnp.bfloat16
WAYS = (True, False)


def pieces_of(rows, widths):
    smallest = min(widths)
    pieces = []
    for a, width in enumerate(widths):
        count = 2 * (width // smallest)
        while rows % (count * 8):
            count //= 2
        pieces += [(a, i * (rows // count), rows // count) for i in range(count)]
    return pieces


def carrier(i, m):
    return (m - 1 - i) % m


def line_kernel(n, m, wq, wk, wv, lq, lk, lv, hq, hk, hv, nt, ns,
                gq, gk, gv, tail_k, tail_v, glow, col_out, norm_out,
                low_q, low_k, low_v, high_q, high_k, high_v, train, step_v, col_ref, norm_ref,
                small_sem, result_sem,
                own_q, own_k, own_v, vec, vec_own,
                send_up, send_dn, recv_up, recv_dn,
                low_send, low_recv, vec_send, vec_recv,
                in_sem, out_sem, low_sem):
    z, x = lax.axis_index("fsdp"), lax.axis_index("width")
    weights, gathered, owns = (wq, wk, wv), (gq, gk, gv), (own_q, own_k, own_v)
    asides = {1: tail_k, 2: tail_v}
    lows, near_lows, near_highs = (lq, lk, lv), (low_q, low_k, low_v), (high_q, high_k, high_v)
    rows = wq.shape[0]
    share = train.shape[1]
    pieces = pieces_of(rows, [w.shape[1] for w in weights])
    count = len(pieces)

    loads = [pltpu.make_async_copy(w, o, in_sem.at[i]) for i, (w, o) in enumerate(zip(weights, owns))]
    smalls = [
        pltpu.make_async_copy(a, b, small_sem.at[i])
        for i, (a, b) in enumerate(zip(lows + (hq, hk, hv, nt, ns), near_lows + near_highs + (train, step_v)))
    ]

    barrier = pltpu.get_barrier_semaphore()
    ends = (z == 0) | (z == n - 1)

    @pl.when(z > 0)
    def _():
        pl.semaphore_signal(barrier, inc=1, device_id_type=MESH, device_id={"fsdp": jnp.maximum(z - 1, 0)})

    @pl.when(z < n - 1)
    def _():
        pl.semaphore_signal(barrier, inc=1, device_id_type=MESH, device_id={"fsdp": jnp.minimum(z + 1, n - 1)})

    for copy in loads + smalls:
        copy.start()

    @pl.when(ends)
    def _():
        pl.semaphore_wait(barrier, 1)

    @pl.when(jnp.logical_not(ends))
    def _():
        pl.semaphore_wait(barrier, 2)

    def sent_block(hop, up):
        return jnp.clip(z - (hop - 1) if up else z + (hop - 1), 0, n - 1)

    def came_block(hop, up):
        return jnp.clip(z - hop if up else z + hop, 0, n - 1)

    def next_on(up):
        return jnp.clip(z + 1 if up else z - 1, 0, n - 1)

    def sends(hop, up):
        return (z >= hop - 1) & (z < n - 1) if up else (z + hop - 1 <= n - 1) & (z > 0)

    def receives(hop, up):
        return z >= hop if up else z + hop <= n - 1

    def travels(hop, c):
        return not (hop == n - 1 and pieces[c][0] in asides)

    def piece(hop, c, up, aside=False):
        a, first, size = pieces[c]
        block = sent_block(hop, up)
        landing = gathered[a].at[block, pl.ds(first, size)]
        source = weights[a].at[pl.ds(first, size)] if hop == 1 else landing
        if aside:
            landing = asides[a].at[pl.ds(first, size)]
        out, back = (send_up, recv_up) if up else (send_dn, recv_dn)
        return pltpu.make_async_remote_copy(
            src_ref=source, dst_ref=landing,
            send_sem=out.at[hop - 1, c], recv_sem=back.at[hop - 1, c],
            device_id={"fsdp": next_on(up)}, device_id_type=MESH,
        )

    def start_piece(hop, c, up):
        if hop == n - 2 and pieces[c][0] in asides:
            aside = (z == n - 3) if up else (z == 2)

            @pl.when(sends(hop, up) & aside)
            def _():
                piece(hop, c, up, True).start()

            @pl.when(sends(hop, up) & jnp.logical_not(aside))
            def _():
                piece(hop, c, up).start()
        else:
            @pl.when(sends(hop, up))
            def _():
                piece(hop, c, up).start()

    def low_piece(hop, i, up):
        block = sent_block(hop, up)
        return pltpu.make_async_remote_copy(
            src_ref=lows[i] if hop == 1 else glow.at[block], dst_ref=glow.at[block],
            send_sem=low_send.at[int(up), hop - 1], recv_sem=low_recv.at[int(up), hop - 1],
            device_id={"fsdp": next_on(up)}, device_id_type=MESH)

    def vec_piece(hop, up):
        block = sent_block(hop, up)
        return pltpu.make_async_remote_copy(
            src_ref=vec_own if hop == 1 else vec.at[block], dst_ref=vec.at[block],
            send_sem=vec_send.at[int(up), hop - 1], recv_sem=vec_recv.at[int(up), hop - 1],
            device_id={"fsdp": next_on(up)}, device_id_type=MESH)

    def carried(i):
        return x == carrier(i, m)

    for c in range(count):
        for up in WAYS:
            start_piece(1, c, up)
    for i in range(3):
        for up in WAYS:
            @pl.when(carried(i) & sends(1, up))
            def _(i=i, up=up):
                low_piece(1, i, up).start()

    for small in smalls:
        small.wait()
    for i in range(3):
        @pl.when(carried(i))
        def _(i=i):
            pltpu.make_async_copy(near_lows[i], glow.at[z], low_sem).start()
    for load in loads:
        load.wait()
    stores = [pltpu.make_async_copy(o, g.at[z], out_sem.at[i]) for i, (g, o) in enumerate(zip(gathered, owns))]
    for store in stores:
        store.start()
    total = col_ref.shape[1]
    tile = 128 if rows % 128 == 0 else rows
    at = 0
    for low, high, own in zip(near_lows, near_highs, owns):
        width = own.shape[1]

        def step(i, best, low=low, high=high, own=own):
            span = pl.ds(pl.multiple_of(i * tile, tile), tile)
            delta = lax.dot_general(
                low[:, span], high[...], (((0,), (0,)), ((), ())), preferred_element_type=F32)
            result = own[span, :].astype(F32) + mix_rate * delta
            return jnp.maximum(best, jnp.max(jnp.abs(result), axis=0, keepdims=True))

        vec_own[:, pl.ds(at, width)] = lax.fori_loop(0, rows // tile, step, jnp.zeros((1, width), F32))
        at += width
    gain = train[...] + step_v[...]
    vec_own[:, pl.ds(total, share)] = gain
    norm_ref[z] = gain
    col_ref[...] = vec_own[:, pl.ds(0, total)]

    for up in WAYS:
        @pl.when(sends(1, up))
        def _(up=up):
            vec_piece(1, up).start()

    results = [pltpu.make_async_copy(col_ref, col_out, result_sem.at[0]),
               pltpu.make_async_copy(norm_ref, norm_out, result_sem.at[1])]
    for hop in range(1, n):
        for up in WAYS:
            @pl.when(receives(hop, up))
            def _(hop=hop, up=up):
                for i in range(3):
                    @pl.when(carried(i))
                    def _(i=i):
                        low_piece(hop, i, up).wait_recv()
                        if hop < n - 1:
                            @pl.when(sends(hop + 1, up))
                            def _():
                                low_piece(hop + 1, i, up).start()
        for c in range(count):
            if not travels(hop, c):
                continue
            for up in WAYS:
                @pl.when(receives(hop, up))
                def _(hop=hop, c=c, up=up):
                    piece(hop, c, up).wait_recv()
                if hop < n - 1 and travels(hop + 1, c):
                    start_piece(hop + 1, c, up)
            if c == 1:
                for up in WAYS:
                    @pl.when(receives(hop, up))
                    def _(hop=hop, up=up):
                        vec_piece(hop, up).wait_recv()
                        if hop < n - 1:
                            @pl.when(sends(hop + 1, up))
                            def _():
                                vec_piece(hop + 1, up).start()
                        block = came_block(hop, up)
                        came = vec[block]
                        col_ref[...] = jnp.maximum(col_ref[...], came[:, :total])
                        norm_ref[block] = came[:, total:total + share]
                if hop == n - 1:
                    for result in results:
                        result.start()
    for copy in stores + results:
        copy.wait()
    for i in range(3):
        @pl.when(carried(i))
        def _(i=i):
            pltpu.make_async_copy(near_lows[i], glow.at[z], low_sem).wait()
    for hop in range(1, n):
        for up in WAYS:
            @pl.when(sends(hop, up))
            def _(hop=hop, up=up):
                vec_piece(hop, up).wait_send()
                for i in range(3):
                    @pl.when(carried(i))
                    def _(i=i):
                        low_piece(hop, i, up).wait_send()
                for c in range(count):
                    if travels(hop, c):
                        piece(hop, c, up).wait_send()


def plane_kernel(m, low_ref, norm_ref, glow, norm, low_send, low_recv, norm_send, norm_recv, own_sem):
    x = lax.axis_index("width")
    barrier = pltpu.get_barrier_semaphore()
    for d in range(1, m):
        pl.semaphore_signal(barrier, inc=1, device_id_type=MESH, device_id={"width": lax.rem(x + d, m)})
    own = pltpu.make_async_copy(norm_ref, norm.at[:, x], own_sem.at[1])
    own.start()
    pl.semaphore_wait(barrier, m - 1)

    def low_to(i, d):
        return pltpu.make_async_remote_copy(
            src_ref=low_ref, dst_ref=glow.at[i], send_sem=low_send.at[i, d - 1], recv_sem=low_recv.at[i],
            device_id={"width": lax.rem(x + d, m)}, device_id_type=MESH)

    def norm_to(d):
        return pltpu.make_async_remote_copy(
            src_ref=norm_ref, dst_ref=norm.at[:, x], send_sem=norm_send.at[d - 1], recv_sem=norm_recv.at[d - 1],
            device_id={"width": lax.rem(x + d, m)}, device_id_type=MESH)

    for i in range(3):
        @pl.when(x == carrier(i, m))
        def _(i=i):
            for d in range(1, m):
                low_to(i, d).start()
            pltpu.make_async_copy(low_ref, glow.at[i], own_sem.at[0]).start()
    for d in range(1, m):
        norm_to(d).start()
    own.wait()
    for d in range(1, m):
        norm_to(d).wait()
    for i in range(3):
        @pl.when(x == carrier(i, m))
        def _(i=i):
            pltpu.make_async_copy(low_ref, glow.at[i], own_sem.at[0]).wait()
            for d in range(1, m):
                low_to(i, d).wait_send()

        @pl.when(x != carrier(i, m))
        def _(i=i):
            low_to(i, 1).wait_recv()


def merged(weight, low, high, scale):
    delta = lax.dot_general(low, high, (((0,), (0,)), ((), ())), preferred_element_type=F32)
    return ((weight.astype(F32) + mix_rate * delta) * scale).astype(BF16)


def merge_kernel(tile, gq, gk, gv, glow, hq, hk, hv, col_q, col_k, col_v, fq, fk, fv, cq, ck, cv):
    arrays = ((gq, hq, col_q, fq), (gk, hk, col_k, fk), (gv, hv, col_v, fv))
    for col, c in ((col_q, cq), (col_k, ck), (col_v, cv)):
        c[...] = col[...]

    def step(t, carry):
        span = pl.ds(pl.multiple_of(t * tile, tile), tile)
        for i, (g, high, col, f) in enumerate(arrays):
            f[span, :] = merged(g[0, span, :], glow[i, 0, :, span], high[...], 1.0 / col[...])
        return carry

    lax.fori_loop(0, gq.shape[1] // tile, step, 0)


def last_kernel(n, parts, came, tail, low_first, low_last, high, col, before, final, out_ref, out_sem):
    z = lax.axis_index("fsdp")
    rows = came.shape[0]
    size = rows // parts

    def store(p, block):
        return pltpu.make_async_copy(
            out_ref.at[pl.ds(p * size, size)],
            final.at[pl.ds(block * rows + p * size, size)], out_sem.at[p])

    def write(source, low, block):
        scale = 1.0 / col[...]
        for p in range(parts):
            span = pl.ds(p * size, size)
            out_ref[span, :] = merged(source[span, :], low[0, 0, :, span], high[...], scale)
            store(p, block).start()
        for p in range(parts):
            store(p, block).wait()

    for at, source, low, block in ((0, came, low_last, n - 1), (1, tail, low_last, n - 1),
                                   (n - 2, tail, low_first, 0), (n - 1, came, low_first, 0)):
        @pl.when(z == at)
        def _(source=source, low=low, block=block):
            write(source, low, block)


def local(n, m, wq, lq, hq, wk, lk, hk, wv, lv, hv, nt, ns):
    rows, cq = wq.shape
    ck, cv = wk.shape[1], wv.shape[1]
    rank, share = hq.shape[0], nt.shape[0]
    total = cq + ck + cv
    length = total + -(-share // 128) * 128
    count = len(pieces_of(rows, [cq, ck, cv]))
    hbm, vmem = pl.BlockSpec(memory_space=pl.ANY), pl.BlockSpec(memory_space=pltpu.VMEM)
    dma = pltpu.SemaphoreType.DMA
    gq, gk, gv, tail_k, tail_v, part, col, normz = pl.pallas_call(
        functools.partial(line_kernel, n, m),
        out_shape=[
            jax.ShapeDtypeStruct((n, rows, cq), BF16),
            jax.ShapeDtypeStruct((n, rows, ck), BF16),
            jax.ShapeDtypeStruct((n, rows, cv), BF16),
            jax.ShapeDtypeStruct((rows, ck), BF16),
            jax.ShapeDtypeStruct((rows, cv), BF16),
            jax.ShapeDtypeStruct((n, rank, rows), BF16),
            jax.ShapeDtypeStruct((1, total), F32),
            jax.ShapeDtypeStruct((n, 1, share), F32),
        ],
        in_specs=[hbm] * 11,
        out_specs=[hbm] * 8,
        scratch_shapes=[
            pltpu.VMEM((rank, rows), BF16), pltpu.VMEM((rank, rows), BF16), pltpu.VMEM((rank, rows), BF16),
            pltpu.VMEM((rank, cq), BF16), pltpu.VMEM((rank, ck), BF16), pltpu.VMEM((rank, cv), BF16),
            pltpu.VMEM((1, share), F32), pltpu.VMEM((1, share), F32),
            pltpu.VMEM((1, total), F32), pltpu.VMEM((n, 1, share), F32), dma((8,)), dma((2,)),
            pltpu.VMEM((rows, cq), BF16), pltpu.VMEM((rows, ck), BF16), pltpu.VMEM((rows, cv), BF16),
            pltpu.VMEM((n, 1, length), F32), pltpu.VMEM((1, length), F32),
            dma((n - 1, count)), dma((n - 1, count)), dma((n - 1, count)), dma((n - 1, count)),
            dma((2, n - 1)), dma((2, n - 1)), dma((2, n - 1)), dma((2, n - 1)),
            dma((3,)), dma((3,)), dma,
        ],
        compiler_params=pltpu.CompilerParams(collective_id=0, has_side_effects=True),
    )(wq, wk, wv, lq.T, lk.T, lv.T, hq, hk, hv, nt.reshape(1, share), ns.reshape(1, share))

    ends = [(1, 0), (n - 2, n - 1)]
    came_k = lax.ppermute(tail_k, "fsdp", ends)
    came_v = lax.ppermute(tail_v, "fsdp", ends)

    glow, norm = pl.pallas_call(
        functools.partial(plane_kernel, m),
        out_shape=[
            jax.ShapeDtypeStruct((3, n, rank, rows), BF16),
            jax.ShapeDtypeStruct((n, m, 1, share), F32),
        ],
        in_specs=[vmem] * 2,
        out_specs=[hbm] * 2,
        scratch_shapes=[dma((3, m - 1)), dma((3,)), dma((m - 1,)), dma((m - 1,)), dma((2,))],
        compiler_params=pltpu.CompilerParams(
            collective_id=1, has_side_effects=True, vmem_limit_bytes=8 * 2**20),
        cost_estimate=pl.CostEstimate(
            flops=2 * n * rows * total * rank, bytes_accessed=n * rows * total, transcendentals=0),
    )(part, normz)

    tile = 128 if rows % 128 == 0 else rows
    halves = 2 if min(cq, ck, cv) % 256 == 0 and ck == cv and cq % ck == 0 else 1
    starts = (0, cq, cq + ck)
    widths = (cq // halves, ck // halves, cv // halves)

    def block(width):
        return pl.BlockSpec((1, rows, width), lambda j, i: (i, 0, j))

    def placed(width):
        return pl.BlockSpec((rows, width), lambda j, i: (i, j))

    def columns(height, width):
        return pl.BlockSpec((height, width), lambda j, i: (0, j))

    def scales(start, width):
        return pl.BlockSpec((1, width), lambda j, i: (0, start // width + j))

    fq, before_k, before_v, col_q, col_k, col_v = pl.pallas_call(
        functools.partial(merge_kernel, tile),
        grid=(halves, n),
        out_shape=[jax.ShapeDtypeStruct((n * rows, c), BF16) for c in (cq, ck, cv)]
        + [jax.ShapeDtypeStruct((1, c), F32) for c in (cq, ck, cv)],
        in_specs=[block(c) for c in widths]
        + [pl.BlockSpec((3, 1, rank, rows), lambda j, i: (0, i, 0, 0))]
        + [columns(rank, c) for c in widths]
        + [scales(start, c) for start, c in zip(starts, widths)],
        out_specs=[placed(c) for c in widths] + [columns(1, c) for c in widths],
        compiler_params=pltpu.CompilerParams(vmem_limit_bytes=60 * 2**20),
        cost_estimate=pl.CostEstimate(
            flops=2 * n * rows * total * rank, bytes_accessed=4 * n * rows * total, transcendentals=0),
    )(gq, gk, gv, glow, hq, hk, hv, col, col, col)

    parts = 7 if rows % (7 * 128) == 0 else 1

    def finish(i, came, tail, high, before):
        width = high.shape[1]
        start = starts[i]
        return pl.pallas_call(
            functools.partial(last_kernel, n, parts),
            grid=(1,),
            out_shape=jax.ShapeDtypeStruct((n * rows, width), BF16),
            in_specs=[vmem, vmem,
                      pl.BlockSpec((1, 1, rank, rows), lambda t: (i, 0, 0, 0)),
                      pl.BlockSpec((1, 1, rank, rows), lambda t: (i, n - 1, 0, 0)),
                      vmem,
                      pl.BlockSpec((1, width), lambda t: (0, start // width)), hbm],
            out_specs=hbm,
            scratch_shapes=[pltpu.VMEM((rows, width), BF16), dma((parts,))],
            input_output_aliases={6: 0},
            compiler_params=pltpu.CompilerParams(vmem_limit_bytes=12 * 2**20),
            cost_estimate=pl.CostEstimate(
                flops=2 * rows * width * rank, bytes_accessed=4 * rows * width, transcendentals=0),
        )(came, tail, glow, glow, high, col, before)

    fk = finish(1, came_k, tail_k, hk, before_k)
    fv = finish(2, came_v, tail_v, hv, before_v)
    return (fq, fk, fv, col_q[0], col_k[0], col_v[0], norm.reshape(-1).astype(BF16))


def solution(mesh):
    placed = (
        P(("trial", "fsdp"), "width"), P(("trial", "fsdp"), None), P("trial", "width"),
        P(("trial", "fsdp"), "width"), P(("trial", "fsdp"), None), P("trial", "width"),
        P(("trial", "fsdp"), "width"), P(("trial", "fsdp"), None), P("trial", "width"),
        P(("trial", "fsdp", "width")), P(("trial", "fsdp", "width")),
    )
    return jax.shard_map(
        functools.partial(local, mesh.shape["fsdp"], mesh.shape["width"]),
        mesh=mesh,
        in_specs=placed,
        out_specs=(
            P("trial", "width"), P("trial", "width"), P("trial", "width"),
            P(("trial", "width")), P(("trial", "width")), P(("trial", "width")),
            P("trial"),
        ),
        check_vma=False,
    )
```

```python
import functools

import jax
import jax.numpy as jnp
from jax import lax
from jax.experimental import pallas as pl
from jax.experimental.pallas import tpu as pltpu
from jax.sharding import PartitionSpec as P

mix_rate = 2.0
MESH = pl.DeviceIdType.MESH
F32, BF16 = jnp.float32, jnp.bfloat16
WAYS = (True, False)


def pieces_of(rows, widths):
    smallest = min(widths)
    pieces = []
    for a, width in enumerate(widths):
        count = 2 * (width // smallest)
        while rows % (count * 8):
            count //= 2
        pieces += [(a, i * (rows // count), rows // count) for i in range(count)]
    return pieces


def carrier(i, m):
    return (m - 1 - i) % m


def line_kernel(n, m, wq, wk, wv, lq, lk, lv, hq, hk, hv, nt, ns,
                gq, gk, gv, tail_k, tail_v, glow, col_out, norm_out,
                low_q, low_k, low_v, high_q, high_k, high_v, train, step_v, col_ref, norm_ref,
                small_sem, result_sem,
                own_q, own_k, own_v, vec, vec_own,
                send_up, send_dn, recv_up, recv_dn,
                low_send, low_recv, vec_send, vec_recv,
                in_sem, out_sem, low_sem, above):
    z, x = lax.axis_index("fsdp"), lax.axis_index("width")
    weights, gathered, owns = (wq, wk, wv), (gq, gk, gv), (own_q, own_k, own_v)
    asides = {1: tail_k, 2: tail_v}
    lows, near_lows, near_highs = (lq, lk, lv), (low_q, low_k, low_v), (high_q, high_k, high_v)
    rows = wq.shape[0]
    share = train.shape[1]
    pieces = pieces_of(rows, [w.shape[1] for w in weights])
    count = len(pieces)

    loads = [pltpu.make_async_copy(w, o, in_sem.at[i]) for i, (w, o) in enumerate(zip(weights, owns))]
    smalls = [
        pltpu.make_async_copy(a, b, small_sem.at[i])
        for i, (a, b) in enumerate(zip(lows + (hq, hk, hv, nt, ns), near_lows + near_highs + (train, step_v)))
    ]

    barrier = pltpu.get_barrier_semaphore()

    @pl.when(z < n - 1)
    def _():
        pl.semaphore_signal(barrier, inc=1, device_id_type=MESH, device_id={"fsdp": jnp.minimum(z + 1, n - 1)})

    for copy in loads + smalls:
        copy.start()

    def sent_block(hop, up):
        return jnp.clip(z - (hop - 1) if up else z + (hop - 1), 0, n - 1)

    def came_block(hop, up):
        return jnp.clip(z - hop if up else z + hop, 0, n - 1)

    def next_on(up):
        return jnp.clip(z + 1 if up else z - 1, 0, n - 1)

    def sends(hop, up):
        return (z >= hop - 1) & (z < n - 1) if up else (z + hop - 1 <= n - 1) & (z > 0)

    def receives(hop, up):
        return z >= hop if up else z + hop <= n - 1

    def travels(hop, c):
        return not (hop == n - 1 and pieces[c][0] in asides)

    def piece(hop, c, up, aside=False):
        a, first, size = pieces[c]
        block = sent_block(hop, up)
        landing = gathered[a].at[block, pl.ds(first, size)]
        source = weights[a].at[pl.ds(first, size)] if hop == 1 else landing
        if aside:
            landing = asides[a].at[pl.ds(first, size)]
        out, back = (send_up, recv_up) if up else (send_dn, recv_dn)
        return pltpu.make_async_remote_copy(
            src_ref=source, dst_ref=landing,
            send_sem=out.at[hop - 1, c], recv_sem=back.at[hop - 1, c],
            device_id={"fsdp": next_on(up)}, device_id_type=MESH,
        )

    def start_piece(hop, c, up):
        if hop == n - 2 and pieces[c][0] in asides:
            aside = (z == n - 3) if up else (z == 2)

            @pl.when(sends(hop, up) & aside)
            def _():
                piece(hop, c, up, True).start()

            @pl.when(sends(hop, up) & jnp.logical_not(aside))
            def _():
                piece(hop, c, up).start()
        else:
            @pl.when(sends(hop, up))
            def _():
                piece(hop, c, up).start()

    def low_piece(hop, i, up):
        block = sent_block(hop, up)
        return pltpu.make_async_remote_copy(
            src_ref=lows[i] if hop == 1 else glow.at[block], dst_ref=glow.at[block],
            send_sem=low_send.at[int(up), hop - 1], recv_sem=low_recv.at[int(up), hop - 1],
            device_id={"fsdp": next_on(up)}, device_id_type=MESH)

    def vec_piece(hop, up):
        block = sent_block(hop, up)
        return pltpu.make_async_remote_copy(
            src_ref=vec_own if hop == 1 else vec.at[block], dst_ref=vec.at[block],
            send_sem=vec_send.at[int(up), hop - 1], recv_sem=vec_recv.at[int(up), hop - 1],
            device_id={"fsdp": next_on(up)}, device_id_type=MESH)

    def carried(i):
        return x == carrier(i, m)

    @pl.when(z > 0)
    def _():
        pl.semaphore_wait(barrier, 1)
        pl.semaphore_signal(above, inc=1, device_id_type=MESH, device_id={"fsdp": jnp.maximum(z - 1, 0)})

    for c in range(count):
        start_piece(1, c, False)

    @pl.when(z < n - 1)
    def _():
        pl.semaphore_wait(above, 1)

    for c in range(count):
        start_piece(1, c, True)
    for i in range(3):
        for up in WAYS:
            @pl.when(carried(i) & sends(1, up))
            def _(i=i, up=up):
                low_piece(1, i, up).start()

    for small in smalls:
        small.wait()
    for i in range(3):
        @pl.when(carried(i))
        def _(i=i):
            pltpu.make_async_copy(near_lows[i], glow.at[z], low_sem).start()
    for load in loads:
        load.wait()
    stores = [pltpu.make_async_copy(o, g.at[z], out_sem.at[i]) for i, (g, o) in enumerate(zip(gathered, owns))]
    for store in stores:
        store.start()
    total = col_ref.shape[1]
    tile = 128 if rows % 128 == 0 else rows
    at = 0
    for low, high, own in zip(near_lows, near_highs, owns):
        width = own.shape[1]

        def step(i, best, low=low, high=high, own=own):
            span = pl.ds(pl.multiple_of(i * tile, tile), tile)
            delta = lax.dot_general(
                low[:, span], high[...], (((0,), (0,)), ((), ())), preferred_element_type=F32)
            result = own[span, :].astype(F32) + mix_rate * delta
            return jnp.maximum(best, jnp.max(jnp.abs(result), axis=0, keepdims=True))

        vec_own[:, pl.ds(at, width)] = lax.fori_loop(0, rows // tile, step, jnp.zeros((1, width), F32))
        at += width
    gain = train[...] + step_v[...]
    vec_own[:, pl.ds(total, share)] = gain
    norm_ref[z] = gain
    col_ref[...] = vec_own[:, pl.ds(0, total)]

    for up in WAYS:
        @pl.when(sends(1, up))
        def _(up=up):
            vec_piece(1, up).start()

    results = [pltpu.make_async_copy(col_ref, col_out, result_sem.at[0]),
               pltpu.make_async_copy(norm_ref, norm_out, result_sem.at[1])]
    for hop in range(1, n):
        for up in WAYS:
            @pl.when(receives(hop, up))
            def _(hop=hop, up=up):
                for i in range(3):
                    @pl.when(carried(i))
                    def _(i=i):
                        low_piece(hop, i, up).wait_recv()
                        if hop < n - 1:
                            @pl.when(sends(hop + 1, up))
                            def _():
                                low_piece(hop + 1, i, up).start()
        for c in range(count):
            if not travels(hop, c):
                continue
            for up in WAYS:
                @pl.when(receives(hop, up))
                def _(hop=hop, c=c, up=up):
                    piece(hop, c, up).wait_recv()
                if hop < n - 1 and travels(hop + 1, c):
                    start_piece(hop + 1, c, up)
            if c == 1:
                for up in WAYS:
                    @pl.when(receives(hop, up))
                    def _(hop=hop, up=up):
                        vec_piece(hop, up).wait_recv()
                        if hop < n - 1:
                            @pl.when(sends(hop + 1, up))
                            def _():
                                vec_piece(hop + 1, up).start()
                        block = came_block(hop, up)
                        came = vec[block]
                        col_ref[...] = jnp.maximum(col_ref[...], came[:, :total])
                        norm_ref[block] = came[:, total:total + share]
                if hop == n - 1:
                    for result in results:
                        result.start()
    for copy in stores + results:
        copy.wait()
    for i in range(3):
        @pl.when(carried(i))
        def _(i=i):
            pltpu.make_async_copy(near_lows[i], glow.at[z], low_sem).wait()
    for hop in range(1, n):
        for up in WAYS:
            @pl.when(sends(hop, up))
            def _(hop=hop, up=up):
                vec_piece(hop, up).wait_send()
                for i in range(3):
                    @pl.when(carried(i))
                    def _(i=i):
                        low_piece(hop, i, up).wait_send()
                for c in range(count):
                    if travels(hop, c):
                        piece(hop, c, up).wait_send()


def plane_kernel(m, low_ref, norm_ref, glow, norm, low_send, low_recv, norm_send, norm_recv, own_sem):
    x = lax.axis_index("width")
    barrier = pltpu.get_barrier_semaphore()
    for d in range(1, m):
        pl.semaphore_signal(barrier, inc=1, device_id_type=MESH, device_id={"width": lax.rem(x + d, m)})
    own = pltpu.make_async_copy(norm_ref, norm.at[:, x], own_sem.at[1])
    own.start()
    pl.semaphore_wait(barrier, m - 1)

    def low_to(i, d):
        return pltpu.make_async_remote_copy(
            src_ref=low_ref, dst_ref=glow.at[i], send_sem=low_send.at[i, d - 1], recv_sem=low_recv.at[i],
            device_id={"width": lax.rem(x + d, m)}, device_id_type=MESH)

    def norm_to(d):
        return pltpu.make_async_remote_copy(
            src_ref=norm_ref, dst_ref=norm.at[:, x], send_sem=norm_send.at[d - 1], recv_sem=norm_recv.at[d - 1],
            device_id={"width": lax.rem(x + d, m)}, device_id_type=MESH)

    for i in range(3):
        @pl.when(x == carrier(i, m))
        def _(i=i):
            for d in range(1, m):
                low_to(i, d).start()
            pltpu.make_async_copy(low_ref, glow.at[i], own_sem.at[0]).start()
    for d in range(1, m):
        norm_to(d).start()
    own.wait()
    for d in range(1, m):
        norm_to(d).wait()
    for i in range(3):
        @pl.when(x == carrier(i, m))
        def _(i=i):
            pltpu.make_async_copy(low_ref, glow.at[i], own_sem.at[0]).wait()
            for d in range(1, m):
                low_to(i, d).wait_send()

        @pl.when(x != carrier(i, m))
        def _(i=i):
            low_to(i, 1).wait_recv()


def merged(weight, low, high, scale):
    delta = lax.dot_general(low, high, (((0,), (0,)), ((), ())), preferred_element_type=F32)
    return ((weight.astype(F32) + mix_rate * delta) * scale).astype(BF16)


def merge_kernel(tile, gq, gk, gv, glow, hq, hk, hv, col_q, col_k, col_v, fq, fk, fv, cq, ck, cv):
    arrays = ((gq, hq, col_q, fq), (gk, hk, col_k, fk), (gv, hv, col_v, fv))
    for col, c in ((col_q, cq), (col_k, ck), (col_v, cv)):
        c[...] = col[...]

    def step(t, carry):
        span = pl.ds(pl.multiple_of(t * tile, tile), tile)
        for i, (g, high, col, f) in enumerate(arrays):
            f[span, :] = merged(g[0, span, :], glow[i, 0, :, span], high[...], 1.0 / col[...])
        return carry

    lax.fori_loop(0, gq.shape[1] // tile, step, 0)


def last_kernel(n, parts, came, tail, low_first, low_last, high, col, before, final, out_ref, out_sem):
    z = lax.axis_index("fsdp")
    rows = came.shape[0]
    size = rows // parts

    def store(p, block):
        return pltpu.make_async_copy(
            out_ref.at[pl.ds(p * size, size)],
            final.at[pl.ds(block * rows + p * size, size)], out_sem.at[p])

    def write(source, low, block):
        scale = 1.0 / col[...]
        for p in range(parts):
            span = pl.ds(p * size, size)
            out_ref[span, :] = merged(source[span, :], low[0, 0, :, span], high[...], scale)
            store(p, block).start()
        for p in range(parts):
            store(p, block).wait()

    for at, source, low, block in ((0, came, low_last, n - 1), (1, tail, low_last, n - 1),
                                   (n - 2, tail, low_first, 0), (n - 1, came, low_first, 0)):
        @pl.when(z == at)
        def _(source=source, low=low, block=block):
            write(source, low, block)


def local(n, m, wq, lq, hq, wk, lk, hk, wv, lv, hv, nt, ns):
    rows, cq = wq.shape
    ck, cv = wk.shape[1], wv.shape[1]
    rank, share = hq.shape[0], nt.shape[0]
    total = cq + ck + cv
    length = total + -(-share // 128) * 128
    count = len(pieces_of(rows, [cq, ck, cv]))
    hbm, vmem = pl.BlockSpec(memory_space=pl.ANY), pl.BlockSpec(memory_space=pltpu.VMEM)
    dma = pltpu.SemaphoreType.DMA
    gq, gk, gv, tail_k, tail_v, part, col, normz = pl.pallas_call(
        functools.partial(line_kernel, n, m),
        out_shape=[
            jax.ShapeDtypeStruct((n, rows, cq), BF16),
            jax.ShapeDtypeStruct((n, rows, ck), BF16),
            jax.ShapeDtypeStruct((n, rows, cv), BF16),
            jax.ShapeDtypeStruct((rows, ck), BF16),
            jax.ShapeDtypeStruct((rows, cv), BF16),
            jax.ShapeDtypeStruct((n, rank, rows), BF16),
            jax.ShapeDtypeStruct((1, total), F32),
            jax.ShapeDtypeStruct((n, 1, share), F32),
        ],
        in_specs=[hbm] * 11,
        out_specs=[hbm] * 8,
        scratch_shapes=[
            pltpu.VMEM((rank, rows), BF16), pltpu.VMEM((rank, rows), BF16), pltpu.VMEM((rank, rows), BF16),
            pltpu.VMEM((rank, cq), BF16), pltpu.VMEM((rank, ck), BF16), pltpu.VMEM((rank, cv), BF16),
            pltpu.VMEM((1, share), F32), pltpu.VMEM((1, share), F32),
            pltpu.VMEM((1, total), F32), pltpu.VMEM((n, 1, share), F32), dma((8,)), dma((2,)),
            pltpu.VMEM((rows, cq), BF16), pltpu.VMEM((rows, ck), BF16), pltpu.VMEM((rows, cv), BF16),
            pltpu.VMEM((n, 1, length), F32), pltpu.VMEM((1, length), F32),
            dma((n - 1, count)), dma((n - 1, count)), dma((n - 1, count)), dma((n - 1, count)),
            dma((2, n - 1)), dma((2, n - 1)), dma((2, n - 1)), dma((2, n - 1)),
            dma((3,)), dma((3,)), dma, pltpu.SemaphoreType.REGULAR,
        ],
        compiler_params=pltpu.CompilerParams(collective_id=0, has_side_effects=True),
    )(wq, wk, wv, lq.T, lk.T, lv.T, hq, hk, hv, nt.reshape(1, share), ns.reshape(1, share))

    ends = [(1, 0), (n - 2, n - 1)]
    came_k = lax.ppermute(tail_k, "fsdp", ends)
    came_v = lax.ppermute(tail_v, "fsdp", ends)

    glow, norm = pl.pallas_call(
        functools.partial(plane_kernel, m),
        out_shape=[
            jax.ShapeDtypeStruct((3, n, rank, rows), BF16),
            jax.ShapeDtypeStruct((n, m, 1, share), F32),
        ],
        in_specs=[vmem] * 2,
        out_specs=[hbm] * 2,
        scratch_shapes=[dma((3, m - 1)), dma((3,)), dma((m - 1,)), dma((m - 1,)), dma((2,))],
        compiler_params=pltpu.CompilerParams(
            collective_id=1, has_side_effects=True, vmem_limit_bytes=8 * 2**20),
        cost_estimate=pl.CostEstimate(
            flops=2 * n * rows * total * rank, bytes_accessed=n * rows * total, transcendentals=0),
    )(part, normz)

    tile = 128 if rows % 128 == 0 else rows
    halves = 2 if min(cq, ck, cv) % 256 == 0 and ck == cv and cq % ck == 0 else 1
    starts = (0, cq, cq + ck)
    widths = (cq // halves, ck // halves, cv // halves)

    def block(width):
        return pl.BlockSpec((1, rows, width), lambda j, i: (i, 0, j))

    def placed(width):
        return pl.BlockSpec((rows, width), lambda j, i: (i, j))

    def columns(height, width):
        return pl.BlockSpec((height, width), lambda j, i: (0, j))

    def scales(start, width):
        return pl.BlockSpec((1, width), lambda j, i: (0, start // width + j))

    fq, before_k, before_v, col_q, col_k, col_v = pl.pallas_call(
        functools.partial(merge_kernel, tile),
        grid=(halves, n),
        out_shape=[jax.ShapeDtypeStruct((n * rows, c), BF16) for c in (cq, ck, cv)]
        + [jax.ShapeDtypeStruct((1, c), F32) for c in (cq, ck, cv)],
        in_specs=[block(c) for c in widths]
        + [pl.BlockSpec((3, 1, rank, rows), lambda j, i: (0, i, 0, 0))]
        + [columns(rank, c) for c in widths]
        + [scales(start, c) for start, c in zip(starts, widths)],
        out_specs=[placed(c) for c in widths] + [columns(1, c) for c in widths],
        compiler_params=pltpu.CompilerParams(vmem_limit_bytes=60 * 2**20),
        cost_estimate=pl.CostEstimate(
            flops=2 * n * rows * total * rank, bytes_accessed=4 * n * rows * total, transcendentals=0),
    )(gq, gk, gv, glow, hq, hk, hv, col, col, col)

    parts = 7 if rows % (7 * 128) == 0 else 1

    def finish(i, came, tail, high, before):
        width = high.shape[1]
        start = starts[i]
        return pl.pallas_call(
            functools.partial(last_kernel, n, parts),
            grid=(1,),
            out_shape=jax.ShapeDtypeStruct((n * rows, width), BF16),
            in_specs=[vmem, vmem,
                      pl.BlockSpec((1, 1, rank, rows), lambda t: (i, 0, 0, 0)),
                      pl.BlockSpec((1, 1, rank, rows), lambda t: (i, n - 1, 0, 0)),
                      vmem,
                      pl.BlockSpec((1, width), lambda t: (0, start // width)), hbm],
            out_specs=hbm,
            scratch_shapes=[pltpu.VMEM((rows, width), BF16), dma((parts,))],
            input_output_aliases={6: 0},
            compiler_params=pltpu.CompilerParams(vmem_limit_bytes=12 * 2**20),
            cost_estimate=pl.CostEstimate(
                flops=2 * rows * width * rank, bytes_accessed=4 * rows * width, transcendentals=0),
        )(came, tail, glow, glow, high, col, before)

    fk = finish(1, came_k, tail_k, hk, before_k)
    fv = finish(2, came_v, tail_v, hv, before_v)
    return (fq, fk, fv, col_q[0], col_k[0], col_v[0], norm.reshape(-1).astype(BF16))


def solution(mesh):
    placed = (
        P(("trial", "fsdp"), "width"), P(("trial", "fsdp"), None), P("trial", "width"),
        P(("trial", "fsdp"), "width"), P(("trial", "fsdp"), None), P("trial", "width"),
        P(("trial", "fsdp"), "width"), P(("trial", "fsdp"), None), P("trial", "width"),
        P(("trial", "fsdp", "width")), P(("trial", "fsdp", "width")),
    )
    return jax.shard_map(
        functools.partial(local, mesh.shape["fsdp"], mesh.shape["width"]),
        mesh=mesh,
        in_specs=placed,
        out_specs=(
            P("trial", "width"), P("trial", "width"), P("trial", "width"),
            P(("trial", "width")), P(("trial", "width")), P(("trial", "width")),
            P("trial"),
        ),
        check_vma=False,
    )
```

```python
import functools

import jax
import jax.numpy as jnp
from jax import lax
from jax.experimental import pallas as pl
from jax.experimental.pallas import tpu as pltpu
from jax.sharding import PartitionSpec as P


mix_rate = 2.0
MESH = pl.DeviceIdType.MESH
F32, BF16 = jnp.float32, jnp.bfloat16
WAYS = (True, False)


def pieces_of(rows, widths):
    smallest = min(widths)
    unit = 128 if rows % 128 == 0 else 8
    units = rows // unit
    pieces = []
    for a, width in enumerate(widths):
        count = min(2 * (width // smallest), units)
        cuts = [unit * (i * units // count) for i in range(count + 1)]
        pieces += [(a, first, last - first) for first, last in zip(cuts, cuts[1:])]
    return pieces


def held_of(pieces):
    return max(c for c, (a, _, _) in enumerate(pieces) if a == 0)


def carrier(i, m):
    return (m - 1 - i) % m


def line_kernel(n, m, trials, wq, wk, wv, lq, lk, lv, hq, hk, hv, nt, ns,
                gq, gk, gv, tail_q, tail_k, tail_v, glow, col_out, norm_out,
                low_q, low_k, low_v, high_q, high_k, high_v, train, step_v, col_ref, norm_ref,
                small_sem, result_sem,
                own_q, own_k, own_v, vec, vec_own,
                send_up, send_dn, recv_up, recv_dn,
                low_send, low_recv, vec_send, vec_recv,
                in_sem, out_sem, low_sem, above):
    z, x = lax.axis_index("fsdp"), lax.axis_index("width")
    weights, gathered, owns = (wq, wk, wv), (gq, gk, gv), (own_q, own_k, own_v)
    asides = (tail_q, tail_k, tail_v)
    late = lax.axis_index("trial") == trials - 1
    lows, near_lows, near_highs = (lq, lk, lv), (low_q, low_k, low_v), (high_q, high_k, high_v)
    rows = wq.shape[0]
    share = train.shape[1]
    pieces = pieces_of(rows, [w.shape[1] for w in weights])
    count = len(pieces)
    spare = held_of(pieces)

    loads = [pltpu.make_async_copy(w, o, in_sem.at[i]) for i, (w, o) in enumerate(zip(weights, owns))]
    smalls = [
        pltpu.make_async_copy(a, b, small_sem.at[i])
        for i, (a, b) in enumerate(zip(lows + (hq, hk, hv, nt, ns), near_lows + near_highs + (train, step_v)))
    ]

    barrier = pltpu.get_barrier_semaphore()

    @pl.when(z < n - 1)
    def _():
        pl.semaphore_signal(barrier, inc=1, device_id_type=MESH, device_id={"fsdp": jnp.minimum(z + 1, n - 1)})

    for copy in loads + smalls:
        copy.start()

    def sent_block(hop, up):
        return jnp.clip(z - (hop - 1) if up else z + (hop - 1), 0, n - 1)

    def came_block(hop, up):
        return jnp.clip(z - hop if up else z + hop, 0, n - 1)

    def next_on(up):
        return jnp.clip(z + 1 if up else z - 1, 0, n - 1)

    def sends(hop, up):
        return (z >= hop - 1) & (z < n - 1) if up else (z + hop - 1 <= n - 1) & (z > 0)

    def receives(hop, up):
        return z >= hop if up else z + hop <= n - 1

    def held(c):
        return late if c == spare else pieces[c][0] > 0

    def travels(hop, c, when):
        if hop < n - 1 or held(c) is False:
            return when
        return False if held(c) is True else when & jnp.logical_not(held(c))

    def piece(hop, c, up, aside=False):
        a, first, size = pieces[c]
        block = sent_block(hop, up)
        landing = gathered[a].at[block, pl.ds(first, size)]
        source = weights[a].at[pl.ds(first, size)] if hop == 1 else landing
        if aside:
            landing = asides[a].at[pl.ds(0 if c == spare else first, size)]
        out, back = (send_up, recv_up) if up else (send_dn, recv_dn)
        return pltpu.make_async_remote_copy(
            src_ref=source, dst_ref=landing,
            send_sem=out.at[hop - 1, c], recv_sem=back.at[hop - 1, c],
            device_id={"fsdp": next_on(up)}, device_id_type=MESH,
        )

    def start_piece(hop, c, up):
        when = travels(hop, c, sends(hop, up))
        if when is False:
            return
        if hop == n - 2 and held(c) is not False:
            aside = (z == n - 3) if up else (z == 2)
            if held(c) is not True:
                aside = aside & held(c)

            @pl.when(when & aside)
            def _():
                piece(hop, c, up, True).start()

            @pl.when(when & jnp.logical_not(aside))
            def _():
                piece(hop, c, up).start()
        else:
            @pl.when(when)
            def _():
                piece(hop, c, up).start()

    def low_piece(hop, i, up):
        block = sent_block(hop, up)
        return pltpu.make_async_remote_copy(
            src_ref=lows[i] if hop == 1 else glow.at[block], dst_ref=glow.at[block],
            send_sem=low_send.at[int(up), hop - 1], recv_sem=low_recv.at[int(up), hop - 1],
            device_id={"fsdp": next_on(up)}, device_id_type=MESH)

    def vec_piece(hop, up):
        block = sent_block(hop, up)
        return pltpu.make_async_remote_copy(
            src_ref=vec_own if hop == 1 else vec.at[block], dst_ref=vec.at[block],
            send_sem=vec_send.at[int(up), hop - 1], recv_sem=vec_recv.at[int(up), hop - 1],
            device_id={"fsdp": next_on(up)}, device_id_type=MESH)

    def carried(i):
        return x == carrier(i, m)

    @pl.when(z > 0)
    def _():
        pl.semaphore_wait(barrier, 1)
        pl.semaphore_signal(above, inc=1, device_id_type=MESH, device_id={"fsdp": jnp.maximum(z - 1, 0)})

    for c in range(count):
        start_piece(1, c, False)

    @pl.when(z < n - 1)
    def _():
        pl.semaphore_wait(above, 1)

    for c in range(count):
        start_piece(1, c, True)
    for i in range(3):
        for up in WAYS:
            @pl.when(carried(i) & sends(1, up))
            def _(i=i, up=up):
                low_piece(1, i, up).start()

    for small in smalls:
        small.wait()
    for i in range(3):
        @pl.when(carried(i))
        def _(i=i):
            pltpu.make_async_copy(near_lows[i], glow.at[z], low_sem).start()
    for load in loads:
        load.wait()
    stores = [pltpu.make_async_copy(o, g.at[z], out_sem.at[i]) for i, (g, o) in enumerate(zip(gathered, owns))]
    for store in stores:
        store.start()
    total = col_ref.shape[1]
    tile = 128 if rows % 128 == 0 else rows
    at = 0
    for low, high, own in zip(near_lows, near_highs, owns):
        width = own.shape[1]

        def step(i, best, low=low, high=high, own=own):
            span = pl.ds(pl.multiple_of(i * tile, tile), tile)
            delta = lax.dot_general(
                low[:, span], high[...], (((0,), (0,)), ((), ())), preferred_element_type=F32)
            result = own[span, :].astype(F32) + mix_rate * delta
            return jnp.maximum(best, jnp.max(jnp.abs(result), axis=0, keepdims=True))

        vec_own[:, pl.ds(at, width)] = lax.fori_loop(0, rows // tile, step, jnp.zeros((1, width), F32))
        at += width
    gain = train[...] + step_v[...]
    vec_own[:, pl.ds(total, share)] = gain
    norm_ref[z] = gain
    col_ref[...] = vec_own[:, pl.ds(0, total)]

    for up in WAYS:
        @pl.when(sends(1, up))
        def _(up=up):
            vec_piece(1, up).start()

    results = [pltpu.make_async_copy(col_ref, col_out, result_sem.at[0]),
               pltpu.make_async_copy(norm_ref, norm_out, result_sem.at[1])]
    for hop in range(1, n):
        for up in WAYS:
            @pl.when(receives(hop, up))
            def _(hop=hop, up=up):
                for i in range(3):
                    @pl.when(carried(i))
                    def _(i=i):
                        low_piece(hop, i, up).wait_recv()
                        if hop < n - 1:
                            @pl.when(sends(hop + 1, up))
                            def _():
                                low_piece(hop + 1, i, up).start()
        for c in range(count):
            if held(c) is True and hop == n - 1:
                continue
            for up in WAYS:
                @pl.when(travels(hop, c, receives(hop, up)))
                def _(hop=hop, c=c, up=up):
                    piece(hop, c, up).wait_recv()

                if hop < n - 1:
                    start_piece(hop + 1, c, up)
            if c == 1:
                for up in WAYS:
                    @pl.when(receives(hop, up))
                    def _(hop=hop, up=up):
                        vec_piece(hop, up).wait_recv()
                        if hop < n - 1:
                            @pl.when(sends(hop + 1, up))
                            def _():
                                vec_piece(hop + 1, up).start()
                        block = came_block(hop, up)
                        came = vec[block]
                        col_ref[...] = jnp.maximum(col_ref[...], came[:, :total])
                        norm_ref[block] = came[:, total:total + share]
                if hop == n - 1:
                    for result in results:
                        result.start()
    for copy in stores + results:
        copy.wait()
    for i in range(3):
        @pl.when(carried(i))
        def _(i=i):
            pltpu.make_async_copy(near_lows[i], glow.at[z], low_sem).wait()
    for hop in range(1, n):
        for up in WAYS:
            @pl.when(sends(hop, up))
            def _(hop=hop, up=up):
                vec_piece(hop, up).wait_send()
                for i in range(3):
                    @pl.when(carried(i))
                    def _(i=i):
                        low_piece(hop, i, up).wait_send()

            for c in range(count):
                if held(c) is True and hop == n - 1:
                    continue

                @pl.when(travels(hop, c, sends(hop, up)))
                def _(hop=hop, c=c, up=up):
                    piece(hop, c, up).wait_send()


def plane_kernel(m, low_ref, norm_ref, glow, norm, low_send, low_recv, norm_send, norm_recv, own_sem):
    x = lax.axis_index("width")
    barrier = pltpu.get_barrier_semaphore()
    for d in range(1, m):
        pl.semaphore_signal(barrier, inc=1, device_id_type=MESH, device_id={"width": lax.rem(x + d, m)})
    own = pltpu.make_async_copy(norm_ref, norm.at[:, x], own_sem.at[1])
    own.start()
    pl.semaphore_wait(barrier, m - 1)

    def low_to(i, d):
        return pltpu.make_async_remote_copy(
            src_ref=low_ref, dst_ref=glow.at[i], send_sem=low_send.at[i, d - 1], recv_sem=low_recv.at[i],
            device_id={"width": lax.rem(x + d, m)}, device_id_type=MESH)

    def norm_to(d):
        return pltpu.make_async_remote_copy(
            src_ref=norm_ref, dst_ref=norm.at[:, x], send_sem=norm_send.at[d - 1], recv_sem=norm_recv.at[d - 1],
            device_id={"width": lax.rem(x + d, m)}, device_id_type=MESH)

    for i in range(3):
        @pl.when(x == carrier(i, m))
        def _(i=i):
            for d in range(1, m):
                low_to(i, d).start()
            pltpu.make_async_copy(low_ref, glow.at[i], own_sem.at[0]).start()
    for d in range(1, m):
        norm_to(d).start()
    own.wait()
    for d in range(1, m):
        norm_to(d).wait()
    for i in range(3):
        @pl.when(x == carrier(i, m))
        def _(i=i):
            pltpu.make_async_copy(low_ref, glow.at[i], own_sem.at[0]).wait()
            for d in range(1, m):
                low_to(i, d).wait_send()

        @pl.when(x != carrier(i, m))
        def _(i=i):
            low_to(i, 1).wait_recv()


def merged(weight, low, high, scale):
    delta = lax.dot_general(low, high, (((0,), (0,)), ((), ())), preferred_element_type=F32)
    return ((weight.astype(F32) + mix_rate * delta) * scale).astype(BF16)


def merge_kernel(tile, gq, gk, gv, glow, hq, hk, hv, col_q, col_k, col_v, fq, fk, fv, cq, ck, cv):
    arrays = ((gq, hq, col_q, fq), (gk, hk, col_k, fk), (gv, hv, col_v, fv))
    for col, c in ((col_q, cq), (col_k, ck), (col_v, cv)):
        c[...] = col[...]

    def step(t, carry):
        span = pl.ds(pl.multiple_of(t * tile, tile), tile)
        for i, (g, high, col, f) in enumerate(arrays):
            f[span, :] = merged(g[0, span, :], glow[i, 0, :, span], high[...], 1.0 / col[...])
        return carry

    lax.fori_loop(0, gq.shape[1] // tile, step, 0)


def last_kernel(n, first, tile, wanted, came, tail, low_first, low_last, high, col, before, final, out_ref, out_sem):
    z = lax.axis_index("fsdp")
    size = came.shape[0]
    rows = low_first.shape[3]

    def store(p, block):
        return pltpu.make_async_copy(
            out_ref.at[pl.ds(p * tile, tile)],
            final.at[pl.ds(block * rows + first + p * tile, tile)], out_sem.at[p])

    def write(source, low, block):
        scale = 1.0 / col[...]
        for p in range(size // tile):
            span = pl.ds(p * tile, tile)
            out_ref[span, :] = merged(source[span, :], low[0, 0, :, pl.ds(first + p * tile, tile)], high[...], scale)
            store(p, block).start()
        for p in range(size // tile):
            store(p, block).wait()

    for at, source, low, block in ((0, came, low_last, n - 1), (1, tail, low_last, n - 1),
                                   (n - 2, tail, low_first, 0), (n - 1, came, low_first, 0)):
        here = z == at
        if wanted is not None:
            here = here & (lax.axis_index("trial") == wanted)

        @pl.when(here)
        def _(source=source, low=low, block=block):
            write(source, low, block)


def local(n, m, trials, wq, lq, hq, wk, lk, hk, wv, lv, hv, nt, ns):
    rows, cq = wq.shape
    ck, cv = wk.shape[1], wv.shape[1]
    rank, share = hq.shape[0], nt.shape[0]
    total = cq + ck + cv
    length = total + -(-share // 128) * 128
    pieces = pieces_of(rows, [cq, ck, cv])
    count, spare = len(pieces), held_of(pieces)
    hbm, vmem = pl.BlockSpec(memory_space=pl.ANY), pl.BlockSpec(memory_space=pltpu.VMEM)
    dma = pltpu.SemaphoreType.DMA
    gq, gk, gv, tail_q, tail_k, tail_v, part, col, normz = pl.pallas_call(
        functools.partial(line_kernel, n, m, trials),
        out_shape=[
            jax.ShapeDtypeStruct((n, rows, cq), BF16),
            jax.ShapeDtypeStruct((n, rows, ck), BF16),
            jax.ShapeDtypeStruct((n, rows, cv), BF16),
            jax.ShapeDtypeStruct((pieces[spare][2], cq), BF16),
            jax.ShapeDtypeStruct((rows, ck), BF16),
            jax.ShapeDtypeStruct((rows, cv), BF16),
            jax.ShapeDtypeStruct((n, rank, rows), BF16),
            jax.ShapeDtypeStruct((1, total), F32),
            jax.ShapeDtypeStruct((n, 1, share), F32),
        ],
        in_specs=[hbm] * 11,
        out_specs=[hbm] * 9,
        scratch_shapes=[
            pltpu.VMEM((rank, rows), BF16), pltpu.VMEM((rank, rows), BF16), pltpu.VMEM((rank, rows), BF16),
            pltpu.VMEM((rank, cq), BF16), pltpu.VMEM((rank, ck), BF16), pltpu.VMEM((rank, cv), BF16),
            pltpu.VMEM((1, share), F32), pltpu.VMEM((1, share), F32),
            pltpu.VMEM((1, total), F32), pltpu.VMEM((n, 1, share), F32), dma((8,)), dma((2,)),
            pltpu.VMEM((rows, cq), BF16), pltpu.VMEM((rows, ck), BF16), pltpu.VMEM((rows, cv), BF16),
            pltpu.VMEM((n, 1, length), F32), pltpu.VMEM((1, length), F32),
            dma((n - 1, count)), dma((n - 1, count)), dma((n - 1, count)), dma((n - 1, count)),
            dma((2, n - 1)), dma((2, n - 1)), dma((2, n - 1)), dma((2, n - 1)),
            dma((3,)), dma((3,)), dma, pltpu.SemaphoreType.REGULAR,
        ],
        compiler_params=pltpu.CompilerParams(collective_id=0, has_side_effects=True),
    )(wq, wk, wv, lq.T, lk.T, lv.T, hq, hk, hv, nt.reshape(1, share), ns.reshape(1, share))

    ends = [(1, 0), (n - 2, n - 1)]
    lone = [(a * trials + trials - 1, b * trials + trials - 1) for a, b in ends]
    came_q = lax.ppermute(tail_q, ("fsdp", "trial"), lone)
    came_k = lax.ppermute(tail_k, "fsdp", ends)
    came_v = lax.ppermute(tail_v, "fsdp", ends)

    glow, norm = pl.pallas_call(
        functools.partial(plane_kernel, m),
        out_shape=[
            jax.ShapeDtypeStruct((3, n, rank, rows), BF16),
            jax.ShapeDtypeStruct((n, m, 1, share), F32),
        ],
        in_specs=[vmem] * 2,
        out_specs=[hbm] * 2,
        scratch_shapes=[dma((3, m - 1)), dma((3,)), dma((m - 1,)), dma((m - 1,)), dma((2,))],
        compiler_params=pltpu.CompilerParams(
            collective_id=1, has_side_effects=True, vmem_limit_bytes=8 * 2**20),
        cost_estimate=pl.CostEstimate(
            flops=2 * n * rows * total * rank, bytes_accessed=n * rows * total, transcendentals=0),
    )(part, normz)

    tile = 128 if rows % 128 == 0 else rows
    halves = 2 if min(cq, ck, cv) % 256 == 0 and ck == cv and cq % ck == 0 else 1
    starts = (0, cq, cq + ck)
    widths = (cq // halves, ck // halves, cv // halves)

    def block(width):
        return pl.BlockSpec((1, rows, width), lambda j, i: (i, 0, j))

    def placed(width):
        return pl.BlockSpec((rows, width), lambda j, i: (i, j))

    def columns(height, width):
        return pl.BlockSpec((height, width), lambda j, i: (0, j))

    def scales(start, width):
        return pl.BlockSpec((1, width), lambda j, i: (0, start // width + j))

    before_q, before_k, before_v, col_q, col_k, col_v = pl.pallas_call(
        functools.partial(merge_kernel, tile),
        grid=(halves, n),
        out_shape=[jax.ShapeDtypeStruct((n * rows, c), BF16) for c in (cq, ck, cv)]
        + [jax.ShapeDtypeStruct((1, c), F32) for c in (cq, ck, cv)],
        in_specs=[block(c) for c in widths]
        + [pl.BlockSpec((3, 1, rank, rows), lambda j, i: (0, i, 0, 0))]
        + [columns(rank, c) for c in widths]
        + [scales(start, c) for start, c in zip(starts, widths)],
        out_specs=[placed(c) for c in widths] + [columns(1, c) for c in widths],
        compiler_params=pltpu.CompilerParams(vmem_limit_bytes=60 * 2**20),
        cost_estimate=pl.CostEstimate(
            flops=2 * n * rows * total * rank, bytes_accessed=4 * n * rows * total, transcendentals=0),
    )(gq, gk, gv, glow, hq, hk, hv, col, col, col)

    def finish(i, came, tail, high, before, first, wanted):
        size, width = came.shape
        step = 128 if rows % 128 == 0 else size
        start = starts[i]
        return pl.pallas_call(
            functools.partial(last_kernel, n, first, step, wanted),
            grid=(1,),
            out_shape=jax.ShapeDtypeStruct((n * rows, width), BF16),
            in_specs=[vmem, vmem,
                      pl.BlockSpec((1, 1, rank, rows), lambda t: (i, 0, 0, 0)),
                      pl.BlockSpec((1, 1, rank, rows), lambda t: (i, n - 1, 0, 0)),
                      vmem,
                      pl.BlockSpec((1, width), lambda t: (0, start // width)), hbm],
            out_specs=hbm,
            scratch_shapes=[pltpu.VMEM((size, width), BF16), dma((size // step,))],
            input_output_aliases={6: 0},
            compiler_params=pltpu.CompilerParams(vmem_limit_bytes=12 * 2**20),
            cost_estimate=pl.CostEstimate(
                flops=2 * size * width * rank, bytes_accessed=4 * size * width, transcendentals=0),
        )(came, tail, glow, glow, high, col, before)

    fq = finish(0, came_q, tail_q, hq, before_q, pieces[spare][1], trials - 1)
    fk = finish(1, came_k, tail_k, hk, before_k, 0, None)
    fv = finish(2, came_v, tail_v, hv, before_v, 0, None)
    return (fq, fk, fv, col_q[0], col_k[0], col_v[0], norm.reshape(-1).astype(BF16))


def solution(mesh):
    placed = (
        P(("trial", "fsdp"), "width"), P(("trial", "fsdp"), None), P("trial", "width"),
        P(("trial", "fsdp"), "width"), P(("trial", "fsdp"), None), P("trial", "width"),
        P(("trial", "fsdp"), "width"), P(("trial", "fsdp"), None), P("trial", "width"),
        P(("trial", "fsdp", "width")), P(("trial", "fsdp", "width")),
    )
    return jax.shard_map(
        functools.partial(local, mesh.shape["fsdp"], mesh.shape["width"], mesh.shape["trial"]),
        mesh=mesh,
        in_specs=placed,
        out_specs=(
            P("trial", "width"), P("trial", "width"), P("trial", "width"),
            P(("trial", "width")), P(("trial", "width")), P(("trial", "width")),
            P("trial"),
        ),
        check_vma=False,
    )
```

```python
import functools

import jax
import jax.numpy as jnp
from jax import lax
from jax.experimental import pallas as pl
from jax.experimental.pallas import tpu as pltpu
from jax.sharding import PartitionSpec as P


mix_rate = 2.0
MESH = pl.DeviceIdType.MESH
F32, BF16 = jnp.float32, jnp.bfloat16
WAYS = (True, False)


def pieces_of(rows, widths):
    smallest = min(widths)
    unit = 128 if rows % 128 == 0 else 8
    units = rows // unit
    pieces = []
    for a, width in enumerate(widths):
        count = min(2 * (width // smallest), units)
        cuts = [unit * (i * units // count) for i in range(count + 1)]
        pieces += [(a, first, last - first) for first, last in zip(cuts, cuts[1:])]
    return pieces


def held_of(pieces):
    return max(c for c, (a, _, _) in enumerate(pieces) if a == 0)


def carrier(i, m):
    return (m - 1 - i) % m


def line_kernel(n, m, trials, wq, wk, wv, lq, lk, lv, hq, hk, hv, nt, ns,
                gq, gk, gv, tail_q, tail_k, tail_v, glow, col_out, norm_out,
                low_q, low_k, low_v, high_q, high_k, high_v, train, step_v, col_ref, norm_ref,
                small_sem, result_sem,
                own_q, own_k, own_v, vec, vec_own,
                send_up, send_dn, recv_up, recv_dn,
                low_send, low_recv, vec_send, vec_recv,
                in_sem, out_sem, low_sem, above):
    z, x = lax.axis_index("fsdp"), lax.axis_index("width")
    weights, gathered, owns = (wq, wk, wv), (gq, gk, gv), (own_q, own_k, own_v)
    asides = (tail_q, tail_k, tail_v)
    late = lax.axis_index("trial") == trials - 1
    lows, near_lows, near_highs = (lq, lk, lv), (low_q, low_k, low_v), (high_q, high_k, high_v)
    rows = wq.shape[0]
    share = train.shape[1]
    pieces = pieces_of(rows, [w.shape[1] for w in weights])
    count = len(pieces)
    spare = held_of(pieces)

    loads = [pltpu.make_async_copy(w, o, in_sem.at[i]) for i, (w, o) in enumerate(zip(weights, owns))]
    smalls = [
        pltpu.make_async_copy(a, b, small_sem.at[i])
        for i, (a, b) in enumerate(zip(lows + (hq, hk, hv, nt, ns), near_lows + near_highs + (train, step_v)))
    ]

    barrier = pltpu.get_barrier_semaphore()

    @pl.when(z < n - 1)
    def _():
        pl.semaphore_signal(barrier, inc=1, device_id_type=MESH, device_id={"fsdp": jnp.minimum(z + 1, n - 1)})

    for copy in loads + smalls:
        copy.start()

    def sent_block(hop, up):
        return jnp.clip(z - (hop - 1) if up else z + (hop - 1), 0, n - 1)

    def came_block(hop, up):
        return jnp.clip(z - hop if up else z + hop, 0, n - 1)

    def next_on(up):
        return jnp.clip(z + 1 if up else z - 1, 0, n - 1)

    def sends(hop, up):
        return (z >= hop - 1) & (z < n - 1) if up else (z + hop - 1 <= n - 1) & (z > 0)

    def receives(hop, up):
        return z >= hop if up else z + hop <= n - 1

    def held(c):
        return late if c == spare else pieces[c][0] > 0

    def travels(hop, c, when):
        if hop < n - 1 or held(c) is False:
            return when
        return False if held(c) is True else when & jnp.logical_not(held(c))

    def piece(hop, c, up, aside=False):
        a, first, size = pieces[c]
        block = sent_block(hop, up)
        landing = gathered[a].at[block, pl.ds(first, size)]
        source = weights[a].at[pl.ds(first, size)] if hop == 1 else landing
        if aside:
            landing = asides[a].at[pl.ds(0 if c == spare else first, size)]
        out, back = (send_up, recv_up) if up else (send_dn, recv_dn)
        return pltpu.make_async_remote_copy(
            src_ref=source, dst_ref=landing,
            send_sem=out.at[hop - 1, c], recv_sem=back.at[hop - 1, c],
            device_id={"fsdp": next_on(up)}, device_id_type=MESH,
        )

    def start_piece(hop, c, up):
        when = travels(hop, c, sends(hop, up))
        if when is False:
            return
        if hop == n - 2 and held(c) is not False:
            aside = (z == n - 3) if up else (z == 2)
            if held(c) is not True:
                aside = aside & held(c)

            @pl.when(when & aside)
            def _():
                piece(hop, c, up, True).start()

            @pl.when(when & jnp.logical_not(aside))
            def _():
                piece(hop, c, up).start()
        else:
            @pl.when(when)
            def _():
                piece(hop, c, up).start()

    def low_piece(hop, i, up):
        block = sent_block(hop, up)
        return pltpu.make_async_remote_copy(
            src_ref=lows[i] if hop == 1 else glow.at[block], dst_ref=glow.at[block],
            send_sem=low_send.at[int(up), hop - 1], recv_sem=low_recv.at[int(up), hop - 1],
            device_id={"fsdp": next_on(up)}, device_id_type=MESH)

    def vec_piece(hop, up):
        block = sent_block(hop, up)
        return pltpu.make_async_remote_copy(
            src_ref=vec_own if hop == 1 else vec.at[block], dst_ref=vec.at[block],
            send_sem=vec_send.at[int(up), hop - 1], recv_sem=vec_recv.at[int(up), hop - 1],
            device_id={"fsdp": next_on(up)}, device_id_type=MESH)

    def carried(i):
        return x == carrier(i, m)

    @pl.when(z > 0)
    def _():
        pl.semaphore_wait(barrier, 1)
        pl.semaphore_signal(above, inc=1, device_id_type=MESH, device_id={"fsdp": jnp.maximum(z - 1, 0)})

    def start_low(up):
        for i in range(3):
            @pl.when(carried(i) & sends(1, up))
            def _(i=i):
                low_piece(1, i, up).start()

    lead = min(3, count)
    for c in range(lead):
        start_piece(1, c, False)
    start_low(False)

    @pl.when(z < n - 1)
    def _():
        pl.semaphore_wait(above, 1)

    for c in range(lead):
        start_piece(1, c, True)
    start_low(True)

    for small in smalls:
        small.wait()
    for i in range(3):
        @pl.when(carried(i))
        def _(i=i):
            pltpu.make_async_copy(near_lows[i], glow.at[z], low_sem).start()
    for load in loads:
        load.wait()
    stores = [pltpu.make_async_copy(o, g.at[z], out_sem.at[i]) for i, (g, o) in enumerate(zip(gathered, owns))]
    for store in stores:
        store.start()
    total = col_ref.shape[1]
    tile = 128 if rows % 128 == 0 else rows
    at = 0
    for low, high, own in zip(near_lows, near_highs, owns):
        width = own.shape[1]

        def step(i, best, low=low, high=high, own=own):
            span = pl.ds(pl.multiple_of(i * tile, tile), tile)
            delta = lax.dot_general(
                low[:, span], high[...], (((0,), (0,)), ((), ())), preferred_element_type=F32)
            result = own[span, :].astype(F32) + mix_rate * delta
            return jnp.maximum(best, jnp.max(jnp.abs(result), axis=0, keepdims=True))

        vec_own[:, pl.ds(at, width)] = lax.fori_loop(0, rows // tile, step, jnp.zeros((1, width), F32))
        at += width
    gain = train[...] + step_v[...]
    vec_own[:, pl.ds(total, share)] = gain
    norm_ref[z] = gain
    col_ref[...] = vec_own[:, pl.ds(0, total)]

    for up in WAYS:
        @pl.when(sends(1, up))
        def _(up=up):
            vec_piece(1, up).start()

    for c in range(lead, count):
        for up in (False, True):
            start_piece(1, c, up)

    results = [pltpu.make_async_copy(col_ref, col_out, result_sem.at[0]),
               pltpu.make_async_copy(norm_ref, norm_out, result_sem.at[1])]

    def small_turn(hop):
        for up in WAYS:
            @pl.when(receives(hop, up))
            def _(up=up):
                vec_piece(hop, up).wait_recv()
                if hop < n - 1:
                    @pl.when(sends(hop + 1, up))
                    def _():
                        vec_piece(hop + 1, up).start()
                for i in range(3):
                    @pl.when(carried(i))
                    def _(i=i):
                        low_piece(hop, i, up).wait_recv()
                        if hop < n - 1:
                            @pl.when(sends(hop + 1, up))
                            def _():
                                low_piece(hop + 1, i, up).start()
                block = came_block(hop, up)
                came = vec[block]
                col_ref[...] = jnp.maximum(col_ref[...], came[:, :total])
                norm_ref[block] = came[:, total:total + share]
        if hop == n - 1:
            for result in results:
                result.start()

    turn = min(3, spare)
    for hop in range(1, n):
        for c in range(count):
            if held(c) is True and hop == n - 1:
                continue
            for up in WAYS:
                @pl.when(travels(hop, c, receives(hop, up)))
                def _(hop=hop, c=c, up=up):
                    piece(hop, c, up).wait_recv()

                if hop < n - 1:
                    start_piece(hop + 1, c, up)
            if c == turn:
                small_turn(hop)
    for copy in stores + results:
        copy.wait()
    for i in range(3):
        @pl.when(carried(i))
        def _(i=i):
            pltpu.make_async_copy(near_lows[i], glow.at[z], low_sem).wait()
    for hop in range(1, n):
        for up in WAYS:
            @pl.when(sends(hop, up))
            def _(hop=hop, up=up):
                vec_piece(hop, up).wait_send()
                for i in range(3):
                    @pl.when(carried(i))
                    def _(i=i):
                        low_piece(hop, i, up).wait_send()

            for c in range(count):
                if held(c) is True and hop == n - 1:
                    continue

                @pl.when(travels(hop, c, sends(hop, up)))
                def _(hop=hop, c=c, up=up):
                    piece(hop, c, up).wait_send()


def plane_kernel(m, low_ref, norm_ref, glow, norm, low_send, low_recv, norm_send, norm_recv, own_sem):
    x = lax.axis_index("width")
    barrier = pltpu.get_barrier_semaphore()
    for d in range(1, m):
        pl.semaphore_signal(barrier, inc=1, device_id_type=MESH, device_id={"width": lax.rem(x + d, m)})
    own = pltpu.make_async_copy(norm_ref, norm.at[:, x], own_sem.at[1])
    own.start()
    pl.semaphore_wait(barrier, m - 1)

    def low_to(i, d):
        return pltpu.make_async_remote_copy(
            src_ref=low_ref, dst_ref=glow.at[i], send_sem=low_send.at[i, d - 1], recv_sem=low_recv.at[i],
            device_id={"width": lax.rem(x + d, m)}, device_id_type=MESH)

    def norm_to(d):
        return pltpu.make_async_remote_copy(
            src_ref=norm_ref, dst_ref=norm.at[:, x], send_sem=norm_send.at[d - 1], recv_sem=norm_recv.at[d - 1],
            device_id={"width": lax.rem(x + d, m)}, device_id_type=MESH)

    for i in range(3):
        @pl.when(x == carrier(i, m))
        def _(i=i):
            for d in range(1, m):
                low_to(i, d).start()
            pltpu.make_async_copy(low_ref, glow.at[i], own_sem.at[0]).start()
    for d in range(1, m):
        norm_to(d).start()
    own.wait()
    for d in range(1, m):
        norm_to(d).wait()
    for i in range(3):
        @pl.when(x == carrier(i, m))
        def _(i=i):
            pltpu.make_async_copy(low_ref, glow.at[i], own_sem.at[0]).wait()
            for d in range(1, m):
                low_to(i, d).wait_send()

        @pl.when(x != carrier(i, m))
        def _(i=i):
            low_to(i, 1).wait_recv()


def merged(weight, low, high, scale):
    delta = lax.dot_general(low, high, (((0,), (0,)), ((), ())), preferred_element_type=F32)
    return ((weight.astype(F32) + mix_rate * delta) * scale).astype(BF16)


def merge_kernel(tile, gq, gk, gv, glow, hq, hk, hv, col_q, col_k, col_v, fq, fk, fv, cq, ck, cv):
    arrays = ((gq, hq, col_q, fq), (gk, hk, col_k, fk), (gv, hv, col_v, fv))
    for col, c in ((col_q, cq), (col_k, ck), (col_v, cv)):
        c[...] = col[...]

    def step(t, carry):
        span = pl.ds(pl.multiple_of(t * tile, tile), tile)
        for i, (g, high, col, f) in enumerate(arrays):
            f[span, :] = merged(g[0, span, :], glow[i, 0, :, span], high[...], 1.0 / col[...])
        return carry

    lax.fori_loop(0, gq.shape[1] // tile, step, 0)


def last_kernel(n, first, tile, wanted, came, tail, low_first, low_last, high, col, before, final, out_ref, out_sem):
    z = lax.axis_index("fsdp")
    size = came.shape[0]
    rows = low_first.shape[3]

    def store(p, block):
        return pltpu.make_async_copy(
            out_ref.at[pl.ds(p * tile, tile)],
            final.at[pl.ds(block * rows + first + p * tile, tile)], out_sem.at[p])

    def write(source, low, block):
        scale = 1.0 / col[...]
        for p in range(size // tile):
            span = pl.ds(p * tile, tile)
            out_ref[span, :] = merged(source[span, :], low[0, 0, :, pl.ds(first + p * tile, tile)], high[...], scale)
            store(p, block).start()
        for p in range(size // tile):
            store(p, block).wait()

    for at, source, low, block in ((0, came, low_last, n - 1), (1, tail, low_last, n - 1),
                                   (n - 2, tail, low_first, 0), (n - 1, came, low_first, 0)):
        here = z == at
        if wanted is not None:
            here = here & (lax.axis_index("trial") == wanted)

        @pl.when(here)
        def _(source=source, low=low, block=block):
            write(source, low, block)


def local(n, m, trials, wq, lq, hq, wk, lk, hk, wv, lv, hv, nt, ns):
    rows, cq = wq.shape
    ck, cv = wk.shape[1], wv.shape[1]
    rank, share = hq.shape[0], nt.shape[0]
    total = cq + ck + cv
    length = total + -(-share // 128) * 128
    pieces = pieces_of(rows, [cq, ck, cv])
    count, spare = len(pieces), held_of(pieces)
    hbm, vmem = pl.BlockSpec(memory_space=pl.ANY), pl.BlockSpec(memory_space=pltpu.VMEM)
    dma = pltpu.SemaphoreType.DMA
    gq, gk, gv, tail_q, tail_k, tail_v, part, col, normz = pl.pallas_call(
        functools.partial(line_kernel, n, m, trials),
        out_shape=[
            jax.ShapeDtypeStruct((n, rows, cq), BF16),
            jax.ShapeDtypeStruct((n, rows, ck), BF16),
            jax.ShapeDtypeStruct((n, rows, cv), BF16),
            jax.ShapeDtypeStruct((pieces[spare][2], cq), BF16),
            jax.ShapeDtypeStruct((rows, ck), BF16),
            jax.ShapeDtypeStruct((rows, cv), BF16),
            jax.ShapeDtypeStruct((n, rank, rows), BF16),
            jax.ShapeDtypeStruct((1, total), F32),
            jax.ShapeDtypeStruct((n, 1, share), F32),
        ],
        in_specs=[hbm] * 11,
        out_specs=[hbm] * 9,
        scratch_shapes=[
            pltpu.VMEM((rank, rows), BF16), pltpu.VMEM((rank, rows), BF16), pltpu.VMEM((rank, rows), BF16),
            pltpu.VMEM((rank, cq), BF16), pltpu.VMEM((rank, ck), BF16), pltpu.VMEM((rank, cv), BF16),
            pltpu.VMEM((1, share), F32), pltpu.VMEM((1, share), F32),
            pltpu.VMEM((1, total), F32), pltpu.VMEM((n, 1, share), F32), dma((8,)), dma((2,)),
            pltpu.VMEM((rows, cq), BF16), pltpu.VMEM((rows, ck), BF16), pltpu.VMEM((rows, cv), BF16),
            pltpu.VMEM((n, 1, length), F32), pltpu.VMEM((1, length), F32),
            dma((n - 1, count)), dma((n - 1, count)), dma((n - 1, count)), dma((n - 1, count)),
            dma((2, n - 1)), dma((2, n - 1)), dma((2, n - 1)), dma((2, n - 1)),
            dma((3,)), dma((3,)), dma, pltpu.SemaphoreType.REGULAR,
        ],
        compiler_params=pltpu.CompilerParams(collective_id=0, has_side_effects=True),
    )(wq, wk, wv, lq.T, lk.T, lv.T, hq, hk, hv, nt.reshape(1, share), ns.reshape(1, share))

    ends = [(1, 0), (n - 2, n - 1)]
    lone = [(a * trials + trials - 1, b * trials + trials - 1) for a, b in ends]
    came_q = lax.ppermute(tail_q, ("fsdp", "trial"), lone)
    came_k = lax.ppermute(tail_k, "fsdp", ends)
    came_v = lax.ppermute(tail_v, "fsdp", ends)

    glow, norm = pl.pallas_call(
        functools.partial(plane_kernel, m),
        out_shape=[
            jax.ShapeDtypeStruct((3, n, rank, rows), BF16),
            jax.ShapeDtypeStruct((n, m, 1, share), F32),
        ],
        in_specs=[vmem] * 2,
        out_specs=[hbm] * 2,
        scratch_shapes=[dma((3, m - 1)), dma((3,)), dma((m - 1,)), dma((m - 1,)), dma((2,))],
        compiler_params=pltpu.CompilerParams(
            collective_id=1, has_side_effects=True, vmem_limit_bytes=8 * 2**20),
        cost_estimate=pl.CostEstimate(
            flops=2 * n * rows * total * rank, bytes_accessed=n * rows * total, transcendentals=0),
    )(part, normz)

    tile = 128 if rows % 128 == 0 else rows
    halves = 2 if min(cq, ck, cv) % 256 == 0 and ck == cv and cq % ck == 0 else 1
    starts = (0, cq, cq + ck)
    widths = (cq // halves, ck // halves, cv // halves)

    def block(width):
        return pl.BlockSpec((1, rows, width), lambda j, i: (i, 0, j))

    def placed(width):
        return pl.BlockSpec((rows, width), lambda j, i: (i, j))

    def columns(height, width):
        return pl.BlockSpec((height, width), lambda j, i: (0, j))

    def scales(start, width):
        return pl.BlockSpec((1, width), lambda j, i: (0, start // width + j))

    before_q, before_k, before_v, col_q, col_k, col_v = pl.pallas_call(
        functools.partial(merge_kernel, tile),
        grid=(halves, n),
        out_shape=[jax.ShapeDtypeStruct((n * rows, c), BF16) for c in (cq, ck, cv)]
        + [jax.ShapeDtypeStruct((1, c), F32) for c in (cq, ck, cv)],
        in_specs=[block(c) for c in widths]
        + [pl.BlockSpec((3, 1, rank, rows), lambda j, i: (0, i, 0, 0))]
        + [columns(rank, c) for c in widths]
        + [scales(start, c) for start, c in zip(starts, widths)],
        out_specs=[placed(c) for c in widths] + [columns(1, c) for c in widths],
        compiler_params=pltpu.CompilerParams(vmem_limit_bytes=60 * 2**20),
        cost_estimate=pl.CostEstimate(
            flops=2 * n * rows * total * rank, bytes_accessed=4 * n * rows * total, transcendentals=0),
    )(gq, gk, gv, glow, hq, hk, hv, col, col, col)

    def finish(i, came, tail, high, before, first, wanted):
        size, width = came.shape
        step = 128 if rows % 128 == 0 else size
        start = starts[i]
        return pl.pallas_call(
            functools.partial(last_kernel, n, first, step, wanted),
            grid=(1,),
            out_shape=jax.ShapeDtypeStruct((n * rows, width), BF16),
            in_specs=[vmem, vmem,
                      pl.BlockSpec((1, 1, rank, rows), lambda t: (i, 0, 0, 0)),
                      pl.BlockSpec((1, 1, rank, rows), lambda t: (i, n - 1, 0, 0)),
                      vmem,
                      pl.BlockSpec((1, width), lambda t: (0, start // width)), hbm],
            out_specs=hbm,
            scratch_shapes=[pltpu.VMEM((size, width), BF16), dma((size // step,))],
            input_output_aliases={6: 0},
            compiler_params=pltpu.CompilerParams(vmem_limit_bytes=12 * 2**20),
            cost_estimate=pl.CostEstimate(
                flops=2 * size * width * rank, bytes_accessed=4 * size * width, transcendentals=0),
        )(came, tail, glow, glow, high, col, before)

    fq = finish(0, came_q, tail_q, hq, before_q, pieces[spare][1], trials - 1)
    fk = finish(1, came_k, tail_k, hk, before_k, 0, None)
    fv = finish(2, came_v, tail_v, hv, before_v, 0, None)
    return (fq, fk, fv, col_q[0], col_k[0], col_v[0], norm.reshape(-1).astype(BF16))


def solution(mesh):
    placed = (
        P(("trial", "fsdp"), "width"), P(("trial", "fsdp"), None), P("trial", "width"),
        P(("trial", "fsdp"), "width"), P(("trial", "fsdp"), None), P("trial", "width"),
        P(("trial", "fsdp"), "width"), P(("trial", "fsdp"), None), P("trial", "width"),
        P(("trial", "fsdp", "width")), P(("trial", "fsdp", "width")),
    )
    return jax.shard_map(
        functools.partial(local, mesh.shape["fsdp"], mesh.shape["width"], mesh.shape["trial"]),
        mesh=mesh,
        in_specs=placed,
        out_specs=(
            P("trial", "width"), P("trial", "width"), P("trial", "width"),
            P(("trial", "width")), P(("trial", "width")), P(("trial", "width")),
            P("trial"),
        ),
        check_vma=False,
    )
```

```python
import functools

import jax
import jax.numpy as jnp
from jax import lax
from jax.experimental import pallas as pl
from jax.experimental.pallas import tpu as pltpu
from jax.sharding import PartitionSpec as P


mix_rate = 2.0
MESH = pl.DeviceIdType.MESH
F32, BF16 = jnp.float32, jnp.bfloat16
WAYS = (True, False)


def pieces_of(rows, widths):
    smallest = min(widths)
    unit = 128 if rows % 128 == 0 else 8
    units = rows // unit
    pieces = []
    for a, width in enumerate(widths):
        count = min(2 * (width // smallest), units)
        cuts = [i * units // count for i in range(count + 1)]
        if a == 2:
            end = units - max(1, units // 7)
            cuts = sorted({0, (end + 1) // 2, end, units})
        pieces += [(a, unit * first, unit * (last - first)) for first, last in zip(cuts, cuts[1:])]
    return pieces


def held_of(pieces):
    return max(c for c, (a, _, _) in enumerate(pieces) if a == 0)


def carrier(i, m):
    return (m - 1 - i) % m


def line_kernel(n, m, trials, wq, wk, wv, lq, lk, lv, hq, hk, hv, nt, ns,
                gq, gk, gv, tail_q, tail_k, tail_v, tail_w, glow, col_out, norm_out,
                low_q, low_k, low_v, high_q, high_k, high_v, train, step_v, col_ref, norm_ref,
                small_sem, result_sem,
                own_q, own_k, own_v, came, leaving, vec_own,
                send_up, send_dn, recv_up, recv_dn,
                low_send, low_recv, vec_send, vec_recv,
                in_sem, out_sem, low_sem, above):
    z, x = lax.axis_index("fsdp"), lax.axis_index("width")
    weights, gathered, owns = (wq, wk, wv), (gq, gk, gv), (own_q, own_k, own_v)
    late = lax.axis_index("trial") == trials - 1
    lows, near_lows, near_highs = (lq, lk, lv), (low_q, low_k, low_v), (high_q, high_k, high_v)
    rows = wq.shape[0]
    share = train.shape[1]
    pieces = pieces_of(rows, [w.shape[1] for w in weights])
    count = len(pieces)
    spare = held_of(pieces)

    def aside_of(c):
        a, first, size = pieces[c]
        if c == spare or c == count - 1:
            return (tail_q if c == spare else tail_w).at[pl.ds(0, size)]
        return (tail_k if a == 1 else tail_v).at[pl.ds(first, size)]

    loads = [pltpu.make_async_copy(w, o, in_sem.at[i]) for i, (w, o) in enumerate(zip(weights, owns))]
    smalls = [
        pltpu.make_async_copy(a, b, small_sem.at[i])
        for i, (a, b) in enumerate(zip(lows + (hq, hk, hv, nt, ns), near_lows + near_highs + (train, step_v)))
    ]

    barrier = pltpu.get_barrier_semaphore()

    @pl.when(z < n - 1)
    def _():
        pl.semaphore_signal(barrier, inc=1, device_id_type=MESH, device_id={"fsdp": jnp.minimum(z + 1, n - 1)})

    def sent_block(hop, up):
        return jnp.clip(z - (hop - 1) if up else z + (hop - 1), 0, n - 1)

    def next_on(up):
        return jnp.clip(z + 1 if up else z - 1, 0, n - 1)

    def sends(hop, up):
        return (z >= hop - 1) & (z < n - 1) if up else (z + hop - 1 <= n - 1) & (z > 0)

    def receives(hop, up):
        return z >= hop if up else z + hop <= n - 1

    def held(c):
        return late if c == spare else pieces[c][0] > 0

    def travels(hop, c, when):
        if hop < n - 1 or held(c) is False:
            return when
        return False if held(c) is True else when & jnp.logical_not(held(c))

    def piece(hop, c, up, aside=False):
        a, first, size = pieces[c]
        block = sent_block(hop, up)
        landing = gathered[a].at[block, pl.ds(first, size)]
        source = weights[a].at[pl.ds(first, size)] if hop == 1 else landing
        if aside:
            landing = aside_of(c)
        out, back = (send_up, recv_up) if up else (send_dn, recv_dn)
        return pltpu.make_async_remote_copy(
            src_ref=source, dst_ref=landing,
            send_sem=out.at[hop - 1, c], recv_sem=back.at[hop - 1, c],
            device_id={"fsdp": next_on(up)}, device_id_type=MESH,
        )

    def start_piece(hop, c, up):
        when = travels(hop, c, sends(hop, up))
        if when is False:
            return
        if hop == n - 2 and held(c) is not False:
            aside = (z == n - 3) if up else (z == 2)
            if held(c) is not True:
                aside = aside & held(c)

            @pl.when(when & aside)
            def _():
                piece(hop, c, up, True).start()

            @pl.when(when & jnp.logical_not(aside))
            def _():
                piece(hop, c, up).start()
        else:
            @pl.when(when)
            def _():
                piece(hop, c, up).start()

    def low_piece(hop, i, up):
        block = sent_block(hop, up)
        return pltpu.make_async_remote_copy(
            src_ref=lows[i] if hop == 1 else glow.at[block], dst_ref=glow.at[block],
            send_sem=low_send.at[int(up), hop - 1], recv_sem=low_recv.at[int(up), hop - 1],
            device_id={"fsdp": next_on(up)}, device_id_type=MESH)

    def message(up, first=False):
        return pltpu.make_async_remote_copy(
            src_ref=vec_own if first else leaving.at[int(up)], dst_ref=came.at[int(up)],
            send_sem=vec_send.at[int(up)], recv_sem=vec_recv.at[int(up)],
            device_id={"fsdp": next_on(up)}, device_id_type=MESH)

    def carried(i):
        return x == carrier(i, m)

    @pl.when(z > 0)
    def _():
        pl.semaphore_wait(barrier, 1)
        pl.semaphore_signal(above, inc=1, device_id_type=MESH, device_id={"fsdp": jnp.maximum(z - 1, 0)})

    def start_low(up):
        for i in range(3):
            @pl.when(carried(i) & sends(1, up))
            def _(i=i):
                low_piece(1, i, up).start()

    lead = min(3, count)
    for c in range(lead):
        start_piece(1, c, False)
    start_low(False)

    @pl.when(z < n - 1)
    def _():
        pl.semaphore_wait(above, 1)

    for c in range(lead):
        start_piece(1, c, True)
    start_low(True)

    for copy in loads + smalls:
        copy.start()
    for small in smalls:
        small.wait()
    for i in range(3):
        @pl.when(carried(i))
        def _(i=i):
            pltpu.make_async_copy(near_lows[i], glow.at[z], low_sem).start()
    for load in loads:
        load.wait()
    stores = [pltpu.make_async_copy(o, g.at[z], out_sem.at[i]) for i, (g, o) in enumerate(zip(gathered, owns))]
    for store in stores:
        store.start()
    total = col_ref.shape[1]
    slot = (vec_own.shape[1] - total) // n
    vec_own[...] = jnp.zeros_like(vec_own)
    tile = 128 if rows % 128 == 0 else rows
    at = 0
    for low, high, own in zip(near_lows, near_highs, owns):
        width = own.shape[1]

        def step(i, best, low=low, high=high, own=own):
            span = pl.ds(pl.multiple_of(i * tile, tile), tile)
            delta = lax.dot_general(
                low[:, span], high[...], (((0,), (0,)), ((), ())), preferred_element_type=F32)
            result = own[span, :].astype(F32) + mix_rate * delta
            return jnp.maximum(best, jnp.max(jnp.abs(result), axis=0, keepdims=True))

        vec_own[:, pl.ds(at, width)] = lax.fori_loop(0, rows // tile, step, jnp.zeros((1, width), F32))
        at += width
    gain = train[...] + step_v[...]
    for b in range(n):
        vec_own[:, pl.ds(total + b * slot, share)] = jnp.where(z == b, gain, 0.0)

    @pl.when(z == 0)
    def _():
        message(True, True).start()

    @pl.when(z == n - 1)
    def _():
        message(False, True).start()

    for c in range(lead, count):
        for up in (False, True):
            start_piece(1, c, up)

    results = [pltpu.make_async_copy(col_ref, col_out, result_sem.at[0]),
               pltpu.make_async_copy(norm_ref, norm_out, result_sem.at[1])]

    def join(mine, other):
        peak = jnp.maximum(mine[:, :total], other[:, :total])
        return jnp.concatenate([peak, mine[:, total:] + other[:, total:]], axis=1)

    def small_turn(hop):
        for up in WAYS:
            @pl.when((z == hop) if up else (z == n - 1 - hop))
            def _(up=up):
                message(up).wait_recv()

                @pl.when((z < n - 1) if up else (z > 0))
                def _():
                    leaving[int(up)] = join(vec_own[...], came[int(up)])
                    message(up).start()

            @pl.when(receives(hop, up))
            def _(up=up):
                for i in range(3):
                    @pl.when(carried(i))
                    def _(i=i):
                        low_piece(hop, i, up).wait_recv()
                        if hop < n - 1:
                            @pl.when(sends(hop + 1, up))
                            def _():
                                low_piece(hop + 1, i, up).start()
        if hop == n - 1:
            col_ref[...] = vec_own[:, pl.ds(0, total)]
            for b in range(n):
                norm_ref[b] = vec_own[:, pl.ds(total + b * slot, share)]
            for up in WAYS:
                @pl.when((z > 0) if up else (z < n - 1))
                def _(up=up):
                    col_ref[...] = jnp.maximum(col_ref[...], came[int(up), :, pl.ds(0, total)])
                    for b in range(n):
                        norm_ref[b] += came[int(up), :, pl.ds(total + b * slot, share)]
            for result in results:
                result.start()

    turn = min(1, spare)
    for hop in range(1, n):
        for c in range(count):
            if held(c) is True and hop == n - 1:
                continue
            for up in WAYS:
                @pl.when(travels(hop, c, receives(hop, up)))
                def _(hop=hop, c=c, up=up):
                    piece(hop, c, up).wait_recv()

                if hop < n - 1:
                    start_piece(hop + 1, c, up)
            if c == turn:
                small_turn(hop)
    for copy in stores + results:
        copy.wait()

    @pl.when(z < n - 1)
    def _():
        message(True).wait_send()

    @pl.when(z > 0)
    def _():
        message(False).wait_send()

    for i in range(3):
        @pl.when(carried(i))
        def _(i=i):
            pltpu.make_async_copy(near_lows[i], glow.at[z], low_sem).wait()
    for hop in range(1, n):
        for up in WAYS:
            @pl.when(sends(hop, up))
            def _(hop=hop, up=up):
                for i in range(3):
                    @pl.when(carried(i))
                    def _(i=i):
                        low_piece(hop, i, up).wait_send()

            for c in range(count):
                if held(c) is True and hop == n - 1:
                    continue

                @pl.when(travels(hop, c, sends(hop, up)))
                def _(hop=hop, c=c, up=up):
                    piece(hop, c, up).wait_send()


def plane_kernel(m, low_ref, norm_ref, glow, norm, low_send, low_recv, norm_send, norm_recv, own_sem):
    x = lax.axis_index("width")
    barrier = pltpu.get_barrier_semaphore()
    for d in range(1, m):
        pl.semaphore_signal(barrier, inc=1, device_id_type=MESH, device_id={"width": lax.rem(x + d, m)})
    own = pltpu.make_async_copy(norm_ref, norm.at[:, x], own_sem.at[1])
    own.start()
    pl.semaphore_wait(barrier, m - 1)

    def low_to(i, d):
        return pltpu.make_async_remote_copy(
            src_ref=low_ref, dst_ref=glow.at[i], send_sem=low_send.at[i, d - 1], recv_sem=low_recv.at[i],
            device_id={"width": lax.rem(x + d, m)}, device_id_type=MESH)

    def norm_to(d):
        return pltpu.make_async_remote_copy(
            src_ref=norm_ref, dst_ref=norm.at[:, x], send_sem=norm_send.at[d - 1], recv_sem=norm_recv.at[d - 1],
            device_id={"width": lax.rem(x + d, m)}, device_id_type=MESH)

    for i in range(3):
        @pl.when(x == carrier(i, m))
        def _(i=i):
            for d in range(1, m):
                low_to(i, d).start()
            pltpu.make_async_copy(low_ref, glow.at[i], own_sem.at[0]).start()
    for d in range(1, m):
        norm_to(d).start()
    own.wait()
    for d in range(1, m):
        norm_to(d).wait()
    for i in range(3):
        @pl.when(x == carrier(i, m))
        def _(i=i):
            pltpu.make_async_copy(low_ref, glow.at[i], own_sem.at[0]).wait()
            for d in range(1, m):
                low_to(i, d).wait_send()

        @pl.when(x != carrier(i, m))
        def _(i=i):
            low_to(i, 1).wait_recv()


def merged(weight, low, high, scale):
    delta = lax.dot_general(low, high, (((0,), (0,)), ((), ())), preferred_element_type=F32)
    return ((weight.astype(F32) + mix_rate * delta) * scale).astype(BF16)


def merge_kernel(tile, gq, gk, gv, glow, hq, hk, hv, col_q, col_k, col_v, fq, fk, fv, cq, ck, cv):
    arrays = ((gq, hq, col_q, fq), (gk, hk, col_k, fk), (gv, hv, col_v, fv))
    for col, c in ((col_q, cq), (col_k, ck), (col_v, cv)):
        c[...] = col[...]

    def step(t, carry):
        span = pl.ds(pl.multiple_of(t * tile, tile), tile)
        for i, (g, high, col, f) in enumerate(arrays):
            f[span, :] = merged(g[0, span, :], glow[i, 0, :, span], high[...], 1.0 / col[...])
        return carry

    lax.fori_loop(0, gq.shape[1] // tile, step, 0)


def last_kernel(n, first, tile, wanted, came, tail, low_first, low_last, high, col, before, final, out_ref, out_sem):
    z = lax.axis_index("fsdp")
    size = came.shape[0]
    rows = low_first.shape[3]

    def store(p, block):
        return pltpu.make_async_copy(
            out_ref.at[pl.ds(p * tile, tile)],
            final.at[pl.ds(block * rows + first + p * tile, tile)], out_sem.at[p])

    def write(source, low, block):
        scale = 1.0 / col[...]
        for p in range(size // tile):
            span = pl.ds(p * tile, tile)
            out_ref[span, :] = merged(source[span, :], low[0, 0, :, pl.ds(first + p * tile, tile)], high[...], scale)
            store(p, block).start()
        for p in range(size // tile):
            store(p, block).wait()

    for at, source, low, block in ((0, came, low_last, n - 1), (1, tail, low_last, n - 1),
                                   (n - 2, tail, low_first, 0), (n - 1, came, low_first, 0)):
        here = z == at
        if wanted is not None:
            here = here & (lax.axis_index("trial") == wanted)

        @pl.when(here)
        def _(source=source, low=low, block=block):
            write(source, low, block)


def local(n, m, trials, wq, lq, hq, wk, lk, hk, wv, lv, hv, nt, ns):
    rows, cq = wq.shape
    ck, cv = wk.shape[1], wv.shape[1]
    rank, share = hq.shape[0], nt.shape[0]
    total = cq + ck + cv
    length = total + n * (-(-share // 128) * 128)
    pieces = pieces_of(rows, [cq, ck, cv])
    count, spare = len(pieces), held_of(pieces)
    hbm, vmem = pl.BlockSpec(memory_space=pl.ANY), pl.BlockSpec(memory_space=pltpu.VMEM)
    dma = pltpu.SemaphoreType.DMA
    gq, gk, gv, tail_q, tail_k, tail_v, tail_w, part, col, normz = pl.pallas_call(
        functools.partial(line_kernel, n, m, trials),
        out_shape=[
            jax.ShapeDtypeStruct((n, rows, cq), BF16),
            jax.ShapeDtypeStruct((n, rows, ck), BF16),
            jax.ShapeDtypeStruct((n, rows, cv), BF16),
            jax.ShapeDtypeStruct((pieces[spare][2], cq), BF16),
            jax.ShapeDtypeStruct((rows, ck), BF16),
            jax.ShapeDtypeStruct((rows - pieces[-1][2], cv), BF16),
            jax.ShapeDtypeStruct((pieces[-1][2], cv), BF16),
            jax.ShapeDtypeStruct((n, rank, rows), BF16),
            jax.ShapeDtypeStruct((1, total), F32),
            jax.ShapeDtypeStruct((n, 1, share), F32),
        ],
        in_specs=[hbm] * 11,
        out_specs=[hbm] * 10,
        scratch_shapes=[
            pltpu.VMEM((rank, rows), BF16), pltpu.VMEM((rank, rows), BF16), pltpu.VMEM((rank, rows), BF16),
            pltpu.VMEM((rank, cq), BF16), pltpu.VMEM((rank, ck), BF16), pltpu.VMEM((rank, cv), BF16),
            pltpu.VMEM((1, share), F32), pltpu.VMEM((1, share), F32),
            pltpu.VMEM((1, total), F32), pltpu.VMEM((n, 1, share), F32), dma((8,)), dma((2,)),
            pltpu.VMEM((rows, cq), BF16), pltpu.VMEM((rows, ck), BF16), pltpu.VMEM((rows, cv), BF16),
            pltpu.VMEM((2, 1, length), F32), pltpu.VMEM((2, 1, length), F32), pltpu.VMEM((1, length), F32),
            dma((n - 1, count)), dma((n - 1, count)), dma((n - 1, count)), dma((n - 1, count)),
            dma((2, n - 1)), dma((2, n - 1)), dma((2,)), dma((2,)),
            dma((3,)), dma((3,)), dma, pltpu.SemaphoreType.REGULAR,
        ],
        compiler_params=pltpu.CompilerParams(collective_id=0, has_side_effects=True),
    )(wq, wk, wv, lq.T, lk.T, lv.T, hq, hk, hv, nt.reshape(1, share), ns.reshape(1, share))

    ends = [(1, 0), (n - 2, n - 1)]
    lone = [(a * trials + trials - 1, b * trials + trials - 1) for a, b in ends]
    came_q = lax.ppermute(tail_q, ("fsdp", "trial"), lone)
    came_k = lax.ppermute(tail_k, "fsdp", ends)
    came_v = lax.ppermute(tail_v, "fsdp", ends)
    came_w = lax.ppermute(tail_w, "fsdp", ends)

    glow, norm = pl.pallas_call(
        functools.partial(plane_kernel, m),
        out_shape=[
            jax.ShapeDtypeStruct((3, n, rank, rows), BF16),
            jax.ShapeDtypeStruct((n, m, 1, share), F32),
        ],
        in_specs=[vmem] * 2,
        out_specs=[hbm] * 2,
        scratch_shapes=[dma((3, m - 1)), dma((3,)), dma((m - 1,)), dma((m - 1,)), dma((2,))],
        compiler_params=pltpu.CompilerParams(
            collective_id=1, has_side_effects=True, vmem_limit_bytes=8 * 2**20),
        cost_estimate=pl.CostEstimate(
            flops=2 * n * rows * total * rank, bytes_accessed=n * rows * total, transcendentals=0),
    )(part, normz)

    tile = 128 if rows % 128 == 0 else rows
    halves = 2 if min(cq, ck, cv) % 256 == 0 and ck == cv and cq % ck == 0 else 1
    starts = (0, cq, cq + ck)
    widths = (cq // halves, ck // halves, cv // halves)

    def block(width):
        return pl.BlockSpec((1, rows, width), lambda j, i: (i, 0, j))

    def placed(width):
        return pl.BlockSpec((rows, width), lambda j, i: (i, j))

    def columns(height, width):
        return pl.BlockSpec((height, width), lambda j, i: (0, j))

    def scales(start, width):
        return pl.BlockSpec((1, width), lambda j, i: (0, start // width + j))

    before_q, before_k, before_v, col_q, col_k, col_v = pl.pallas_call(
        functools.partial(merge_kernel, tile),
        grid=(halves, n),
        out_shape=[jax.ShapeDtypeStruct((n * rows, c), BF16) for c in (cq, ck, cv)]
        + [jax.ShapeDtypeStruct((1, c), F32) for c in (cq, ck, cv)],
        in_specs=[block(c) for c in widths]
        + [pl.BlockSpec((3, 1, rank, rows), lambda j, i: (0, i, 0, 0))]
        + [columns(rank, c) for c in widths]
        + [scales(start, c) for start, c in zip(starts, widths)],
        out_specs=[placed(c) for c in widths] + [columns(1, c) for c in widths],
        compiler_params=pltpu.CompilerParams(vmem_limit_bytes=60 * 2**20),
        cost_estimate=pl.CostEstimate(
            flops=2 * n * rows * total * rank, bytes_accessed=4 * n * rows * total, transcendentals=0),
    )(gq, gk, gv, glow, hq, hk, hv, col, col, col)

    def finish(i, came, tail, high, before, first, wanted):
        size, width = came.shape
        step = 128 if size % 128 == 0 else size
        start = starts[i]
        return pl.pallas_call(
            functools.partial(last_kernel, n, first, step, wanted),
            grid=(1,),
            out_shape=jax.ShapeDtypeStruct((n * rows, width), BF16),
            in_specs=[vmem, vmem,
                      pl.BlockSpec((1, 1, rank, rows), lambda t: (i, 0, 0, 0)),
                      pl.BlockSpec((1, 1, rank, rows), lambda t: (i, n - 1, 0, 0)),
                      vmem,
                      pl.BlockSpec((1, width), lambda t: (0, start // width)), hbm],
            out_specs=hbm,
            scratch_shapes=[pltpu.VMEM((size, width), BF16), dma((size // step,))],
            input_output_aliases={6: 0},
            compiler_params=pltpu.CompilerParams(vmem_limit_bytes=12 * 2**20),
            cost_estimate=pl.CostEstimate(
                flops=2 * size * width * rank, bytes_accessed=4 * size * width, transcendentals=0),
        )(came, tail, glow, glow, high, col, before)

    fq = finish(0, came_q, tail_q, hq, before_q, pieces[spare][1], trials - 1)
    fk = finish(1, came_k, tail_k, hk, before_k, 0, None)
    most = finish(2, came_v, tail_v, hv, before_v, 0, None)
    fv = finish(2, came_w, tail_w, hv, most, pieces[-1][1], None)
    return (fq, fk, fv, col_q[0], col_k[0], col_v[0], norm.reshape(-1).astype(BF16))


def solution(mesh):
    placed = (
        P(("trial", "fsdp"), "width"), P(("trial", "fsdp"), None), P("trial", "width"),
        P(("trial", "fsdp"), "width"), P(("trial", "fsdp"), None), P("trial", "width"),
        P(("trial", "fsdp"), "width"), P(("trial", "fsdp"), None), P("trial", "width"),
        P(("trial", "fsdp", "width")), P(("trial", "fsdp", "width")),
    )
    return jax.shard_map(
        functools.partial(local, mesh.shape["fsdp"], mesh.shape["width"], mesh.shape["trial"]),
        mesh=mesh,
        in_specs=placed,
        out_specs=(
            P("trial", "width"), P("trial", "width"), P("trial", "width"),
            P(("trial", "width")), P(("trial", "width")), P(("trial", "width")),
            P("trial"),
        ),
        check_vma=False,
    )
```

```python
import functools

import jax
import jax.numpy as jnp
from jax import lax
from jax.experimental import pallas as pl
from jax.experimental.pallas import tpu as pltpu
from jax.sharding import PartitionSpec as P


mix_rate = 2.0
MESH = pl.DeviceIdType.MESH
F32, BF16 = jnp.float32, jnp.bfloat16
WAYS = (True, False)


def pieces_of(rows, widths):
    smallest = min(widths)
    unit = 128 if rows % 128 == 0 else 8
    units = rows // unit
    pieces = []
    for a, width in enumerate(widths):
        count = min(2 * (width // smallest), units)
        cuts = [i * units // count for i in range(count + 1)]
        if a == 2:
            end = units - max(1, units // 7)
            cuts = sorted({0, (end + 1) // 2, end, units})
        pieces += [(a, unit * first, unit * (last - first)) for first, last in zip(cuts, cuts[1:])]
    return pieces


def held_of(pieces):
    return max(c for c, (a, _, _) in enumerate(pieces) if a == 0)


def carrier(i, m):
    return (m - 1 - i) % m


def line_kernel(n, m, trials, wq, wk, wv, lq, lk, lv, hq, hk, hv, nt, ns,
                gq, gk, gv, tail_q, tail_k, tail_v, tail_w, glow, col_out, norm_out,
                low_q, low_k, low_v, high_q, high_k, high_v, train, step_v, col_ref, norm_ref,
                small_sem, result_sem,
                own_q, own_k, own_v, came, leaving, vec_own,
                send_up, send_dn, recv_up, recv_dn,
                low_send, low_recv, vec_send, vec_recv,
                in_sem, out_sem, low_sem, inner):
    z, x = lax.axis_index("fsdp"), lax.axis_index("width")
    weights, gathered, owns = (wq, wk, wv), (gq, gk, gv), (own_q, own_k, own_v)
    late = lax.axis_index("trial") == trials - 1
    lows, near_lows, near_highs = (lq, lk, lv), (low_q, low_k, low_v), (high_q, high_k, high_v)
    rows = wq.shape[0]
    share = train.shape[1]
    pieces = pieces_of(rows, [w.shape[1] for w in weights])
    count = len(pieces)
    spare = held_of(pieces)

    def aside_of(c):
        a, first, size = pieces[c]
        if c == spare or c == count - 1:
            return (tail_q if c == spare else tail_w).at[pl.ds(0, size)]
        return (tail_k if a == 1 else tail_v).at[pl.ds(first, size)]

    loads = [pltpu.make_async_copy(w, o, in_sem.at[i]) for i, (w, o) in enumerate(zip(weights, owns))]
    smalls = [
        pltpu.make_async_copy(a, b, small_sem.at[i])
        for i, (a, b) in enumerate(zip(lows + (hq, hk, hv, nt, ns), near_lows + near_highs + (train, step_v)))
    ]

    barrier = pltpu.get_barrier_semaphore()
    middle = n // 2

    def tell(semaphore, when, upward):
        @pl.when(when)
        def _():
            pl.semaphore_signal(semaphore, inc=1, device_id_type=MESH, device_id={
                "fsdp": jnp.minimum(z + 1, n - 1) if upward else jnp.maximum(z - 1, 0)})

    tell(barrier, z < middle, True)
    tell(barrier, z > middle, False)

    def sent_block(hop, up):
        return jnp.clip(z - (hop - 1) if up else z + (hop - 1), 0, n - 1)

    def next_on(up):
        return jnp.clip(z + 1 if up else z - 1, 0, n - 1)

    def sends(hop, up):
        return (z >= hop - 1) & (z < n - 1) if up else (z + hop - 1 <= n - 1) & (z > 0)

    def receives(hop, up):
        return z >= hop if up else z + hop <= n - 1

    def held(c):
        return late if c == spare else pieces[c][0] > 0

    def travels(hop, c, when):
        if hop < n - 1 or held(c) is False:
            return when
        return False if held(c) is True else when & jnp.logical_not(held(c))

    def piece(hop, c, up, aside=False):
        a, first, size = pieces[c]
        block = sent_block(hop, up)
        landing = gathered[a].at[block, pl.ds(first, size)]
        source = weights[a].at[pl.ds(first, size)] if hop == 1 else landing
        if aside:
            landing = aside_of(c)
        out, back = (send_up, recv_up) if up else (send_dn, recv_dn)
        return pltpu.make_async_remote_copy(
            src_ref=source, dst_ref=landing,
            send_sem=out.at[hop - 1, c], recv_sem=back.at[hop - 1, c],
            device_id={"fsdp": next_on(up)}, device_id_type=MESH,
        )

    def start_piece(hop, c, up):
        when = travels(hop, c, sends(hop, up))
        if when is False:
            return
        if hop == n - 2 and held(c) is not False:
            aside = (z == n - 3) if up else (z == 2)
            if held(c) is not True:
                aside = aside & held(c)

            @pl.when(when & aside)
            def _():
                piece(hop, c, up, True).start()

            @pl.when(when & jnp.logical_not(aside))
            def _():
                piece(hop, c, up).start()
        else:
            @pl.when(when)
            def _():
                piece(hop, c, up).start()

    def low_piece(hop, i, up):
        block = sent_block(hop, up)
        return pltpu.make_async_remote_copy(
            src_ref=lows[i] if hop == 1 else glow.at[block], dst_ref=glow.at[block],
            send_sem=low_send.at[int(up), hop - 1], recv_sem=low_recv.at[int(up), hop - 1],
            device_id={"fsdp": next_on(up)}, device_id_type=MESH)

    def message(up, first=False):
        return pltpu.make_async_remote_copy(
            src_ref=vec_own if first else leaving.at[int(up)], dst_ref=came.at[int(up)],
            send_sem=vec_send.at[int(up)], recv_sem=vec_recv.at[int(up)],
            device_id={"fsdp": next_on(up)}, device_id_type=MESH)

    def carried(i):
        return x == carrier(i, m)

    @pl.when((z > 0) & (z < n - 1) & (z != middle))
    def _():
        pl.semaphore_wait(barrier, 1)

    @pl.when(z == middle)
    def _():
        pl.semaphore_wait(barrier, 2 if middle < n - 1 else 1)

    tell(inner, (z > 0) & (z <= middle), False)
    tell(inner, (z >= middle) & (z < n - 1), True)

    def start_low(up):
        for i in range(3):
            @pl.when(carried(i) & sends(1, up))
            def _(i=i):
                low_piece(1, i, up).start()

    lead = min(3, count)

    def start_lead(up):
        for c in range(lead):
            start_piece(1, c, up)
        start_low(up)

    @pl.when(z <= middle)
    def _():
        start_lead(False)

    @pl.when(z >= middle)
    def _():
        start_lead(True)

    @pl.when(z != middle)
    def _():
        pl.semaphore_wait(inner, 1)

    @pl.when(z < middle)
    def _():
        start_lead(True)

    @pl.when(z > middle)
    def _():
        start_lead(False)

    for copy in loads + smalls:
        copy.start()
    for small in smalls:
        small.wait()
    for i in range(3):
        @pl.when(carried(i))
        def _(i=i):
            pltpu.make_async_copy(near_lows[i], glow.at[z], low_sem).start()
    for load in loads:
        load.wait()
    stores = [pltpu.make_async_copy(o, g.at[z], out_sem.at[i]) for i, (g, o) in enumerate(zip(gathered, owns))]
    for store in stores:
        store.start()
    total = col_ref.shape[1]
    slot = (vec_own.shape[1] - total) // n
    vec_own[...] = jnp.zeros_like(vec_own)
    tile = 128 if rows % 128 == 0 else rows
    at = 0
    for low, high, own in zip(near_lows, near_highs, owns):
        width = own.shape[1]

        def step(i, best, low=low, high=high, own=own):
            span = pl.ds(pl.multiple_of(i * tile, tile), tile)
            delta = lax.dot_general(
                low[:, span], high[...], (((0,), (0,)), ((), ())), preferred_element_type=F32)
            result = own[span, :].astype(F32) + mix_rate * delta
            return jnp.maximum(best, jnp.max(jnp.abs(result), axis=0, keepdims=True))

        vec_own[:, pl.ds(at, width)] = lax.fori_loop(0, rows // tile, step, jnp.zeros((1, width), F32))
        at += width
    gain = train[...] + step_v[...]
    for b in range(n):
        vec_own[:, pl.ds(total + b * slot, share)] = jnp.where(z == b, gain, 0.0)

    @pl.when(z == 0)
    def _():
        message(True, True).start()

    @pl.when(z == n - 1)
    def _():
        message(False, True).start()

    for c in range(lead, count):
        for up in (False, True):
            start_piece(1, c, up)

    results = [pltpu.make_async_copy(col_ref, col_out, result_sem.at[0]),
               pltpu.make_async_copy(norm_ref, norm_out, result_sem.at[1])]

    def join(mine, other):
        peak = jnp.maximum(mine[:, :total], other[:, :total])
        return jnp.concatenate([peak, mine[:, total:] + other[:, total:]], axis=1)

    def small_turn(hop):
        for up in WAYS:
            @pl.when((z == hop) if up else (z == n - 1 - hop))
            def _(up=up):
                message(up).wait_recv()

                @pl.when((z < n - 1) if up else (z > 0))
                def _():
                    leaving[int(up)] = join(vec_own[...], came[int(up)])
                    message(up).start()

            @pl.when(receives(hop, up))
            def _(up=up):
                for i in range(3):
                    @pl.when(carried(i))
                    def _(i=i):
                        low_piece(hop, i, up).wait_recv()
                        if hop < n - 1:
                            @pl.when(sends(hop + 1, up))
                            def _():
                                low_piece(hop + 1, i, up).start()
        if hop == n - 1:
            col_ref[...] = vec_own[:, pl.ds(0, total)]
            for b in range(n):
                norm_ref[b] = vec_own[:, pl.ds(total + b * slot, share)]
            for up in WAYS:
                @pl.when((z > 0) if up else (z < n - 1))
                def _(up=up):
                    col_ref[...] = jnp.maximum(col_ref[...], came[int(up), :, pl.ds(0, total)])
                    for b in range(n):
                        norm_ref[b] += came[int(up), :, pl.ds(total + b * slot, share)]
            for result in results:
                result.start()

    turn = min(1, spare)
    for hop in range(1, n):
        for c in range(count):
            if held(c) is True and hop == n - 1:
                continue
            for up in WAYS:
                @pl.when(travels(hop, c, receives(hop, up)))
                def _(hop=hop, c=c, up=up):
                    piece(hop, c, up).wait_recv()

                if hop < n - 1:
                    start_piece(hop + 1, c, up)
            if c == turn:
                small_turn(hop)
    for copy in stores + results:
        copy.wait()

    @pl.when(z < n - 1)
    def _():
        message(True).wait_send()

    @pl.when(z > 0)
    def _():
        message(False).wait_send()

    for i in range(3):
        @pl.when(carried(i))
        def _(i=i):
            pltpu.make_async_copy(near_lows[i], glow.at[z], low_sem).wait()
    for hop in range(1, n):
        for up in WAYS:
            @pl.when(sends(hop, up))
            def _(hop=hop, up=up):
                for i in range(3):
                    @pl.when(carried(i))
                    def _(i=i):
                        low_piece(hop, i, up).wait_send()

            for c in range(count):
                if held(c) is True and hop == n - 1:
                    continue

                @pl.when(travels(hop, c, sends(hop, up)))
                def _(hop=hop, c=c, up=up):
                    piece(hop, c, up).wait_send()


def plane_kernel(m, low_ref, norm_ref, glow, norm, low_send, low_recv, norm_send, norm_recv, own_sem):
    x = lax.axis_index("width")
    barrier = pltpu.get_barrier_semaphore()
    for d in range(1, m):
        pl.semaphore_signal(barrier, inc=1, device_id_type=MESH, device_id={"width": lax.rem(x + d, m)})
    own = pltpu.make_async_copy(norm_ref, norm.at[:, x], own_sem.at[1])
    own.start()
    pl.semaphore_wait(barrier, m - 1)

    def low_to(i, d):
        return pltpu.make_async_remote_copy(
            src_ref=low_ref, dst_ref=glow.at[i], send_sem=low_send.at[i, d - 1], recv_sem=low_recv.at[i],
            device_id={"width": lax.rem(x + d, m)}, device_id_type=MESH)

    def norm_to(d):
        return pltpu.make_async_remote_copy(
            src_ref=norm_ref, dst_ref=norm.at[:, x], send_sem=norm_send.at[d - 1], recv_sem=norm_recv.at[d - 1],
            device_id={"width": lax.rem(x + d, m)}, device_id_type=MESH)

    for i in range(3):
        @pl.when(x == carrier(i, m))
        def _(i=i):
            for d in range(1, m):
                low_to(i, d).start()
            pltpu.make_async_copy(low_ref, glow.at[i], own_sem.at[0]).start()
    for d in range(1, m):
        norm_to(d).start()
    own.wait()
    for d in range(1, m):
        norm_to(d).wait()
    for i in range(3):
        @pl.when(x == carrier(i, m))
        def _(i=i):
            pltpu.make_async_copy(low_ref, glow.at[i], own_sem.at[0]).wait()
            for d in range(1, m):
                low_to(i, d).wait_send()

        @pl.when(x != carrier(i, m))
        def _(i=i):
            low_to(i, 1).wait_recv()


def merged(weight, low, high, scale):
    delta = lax.dot_general(low, high, (((0,), (0,)), ((), ())), preferred_element_type=F32)
    return ((weight.astype(F32) + mix_rate * delta) * scale).astype(BF16)


def merge_kernel(tile, gq, gk, gv, glow, hq, hk, hv, col_q, col_k, col_v, fq, fk, fv, cq, ck, cv):
    arrays = ((gq, hq, col_q, fq), (gk, hk, col_k, fk), (gv, hv, col_v, fv))
    for col, c in ((col_q, cq), (col_k, ck), (col_v, cv)):
        c[...] = col[...]

    def step(t, carry):
        span = pl.ds(pl.multiple_of(t * tile, tile), tile)
        for i, (g, high, col, f) in enumerate(arrays):
            f[span, :] = merged(g[0, span, :], glow[i, 0, :, span], high[...], 1.0 / col[...])
        return carry

    lax.fori_loop(0, gq.shape[1] // tile, step, 0)


def last_kernel(n, first, tile, wanted, came, tail, low_first, low_last, high, col, before, final, out_ref, out_sem):
    z = lax.axis_index("fsdp")
    size = came.shape[0]
    rows = low_first.shape[3]

    def store(p, block):
        return pltpu.make_async_copy(
            out_ref.at[pl.ds(p * tile, tile)],
            final.at[pl.ds(block * rows + first + p * tile, tile)], out_sem.at[p])

    def write(source, low, block):
        scale = 1.0 / col[...]
        for p in range(size // tile):
            span = pl.ds(p * tile, tile)
            out_ref[span, :] = merged(source[span, :], low[0, 0, :, pl.ds(first + p * tile, tile)], high[...], scale)
            store(p, block).start()
        for p in range(size // tile):
            store(p, block).wait()

    for at, source, low, block in ((0, came, low_last, n - 1), (1, tail, low_last, n - 1),
                                   (n - 2, tail, low_first, 0), (n - 1, came, low_first, 0)):
        here = z == at
        if wanted is not None:
            here = here & (lax.axis_index("trial") == wanted)

        @pl.when(here)
        def _(source=source, low=low, block=block):
            write(source, low, block)


def local(n, m, trials, wq, lq, hq, wk, lk, hk, wv, lv, hv, nt, ns):
    rows, cq = wq.shape
    ck, cv = wk.shape[1], wv.shape[1]
    rank, share = hq.shape[0], nt.shape[0]
    total = cq + ck + cv
    length = total + n * (-(-share // 128) * 128)
    pieces = pieces_of(rows, [cq, ck, cv])
    count, spare = len(pieces), held_of(pieces)
    hbm, vmem = pl.BlockSpec(memory_space=pl.ANY), pl.BlockSpec(memory_space=pltpu.VMEM)
    dma = pltpu.SemaphoreType.DMA
    gq, gk, gv, tail_q, tail_k, tail_v, tail_w, part, col, normz = pl.pallas_call(
        functools.partial(line_kernel, n, m, trials),
        out_shape=[
            jax.ShapeDtypeStruct((n, rows, cq), BF16),
            jax.ShapeDtypeStruct((n, rows, ck), BF16),
            jax.ShapeDtypeStruct((n, rows, cv), BF16),
            jax.ShapeDtypeStruct((pieces[spare][2], cq), BF16),
            jax.ShapeDtypeStruct((rows, ck), BF16),
            jax.ShapeDtypeStruct((rows - pieces[-1][2], cv), BF16),
            jax.ShapeDtypeStruct((pieces[-1][2], cv), BF16),
            jax.ShapeDtypeStruct((n, rank, rows), BF16),
            jax.ShapeDtypeStruct((1, total), F32),
            jax.ShapeDtypeStruct((n, 1, share), F32),
        ],
        in_specs=[hbm] * 11,
        out_specs=[hbm] * 10,
        scratch_shapes=[
            pltpu.VMEM((rank, rows), BF16), pltpu.VMEM((rank, rows), BF16), pltpu.VMEM((rank, rows), BF16),
            pltpu.VMEM((rank, cq), BF16), pltpu.VMEM((rank, ck), BF16), pltpu.VMEM((rank, cv), BF16),
            pltpu.VMEM((1, share), F32), pltpu.VMEM((1, share), F32),
            pltpu.VMEM((1, total), F32), pltpu.VMEM((n, 1, share), F32), dma((8,)), dma((2,)),
            pltpu.VMEM((rows, cq), BF16), pltpu.VMEM((rows, ck), BF16), pltpu.VMEM((rows, cv), BF16),
            pltpu.VMEM((2, 1, length), F32), pltpu.VMEM((2, 1, length), F32), pltpu.VMEM((1, length), F32),
            dma((n - 1, count)), dma((n - 1, count)), dma((n - 1, count)), dma((n - 1, count)),
            dma((2, n - 1)), dma((2, n - 1)), dma((2,)), dma((2,)),
            dma((3,)), dma((3,)), dma, pltpu.SemaphoreType.REGULAR,
        ],
        compiler_params=pltpu.CompilerParams(collective_id=0, has_side_effects=True),
    )(wq, wk, wv, lq.T, lk.T, lv.T, hq, hk, hv, nt.reshape(1, share), ns.reshape(1, share))

    ends = [(1, 0), (n - 2, n - 1)]
    lone = [(a * trials + trials - 1, b * trials + trials - 1) for a, b in ends]
    came_q = lax.ppermute(tail_q, ("fsdp", "trial"), lone)
    came_k = lax.ppermute(tail_k, "fsdp", ends)
    came_v = lax.ppermute(tail_v, "fsdp", ends)
    came_w = lax.ppermute(tail_w, "fsdp", ends)

    glow, norm = pl.pallas_call(
        functools.partial(plane_kernel, m),
        out_shape=[
            jax.ShapeDtypeStruct((3, n, rank, rows), BF16),
            jax.ShapeDtypeStruct((n, m, 1, share), F32),
        ],
        in_specs=[vmem] * 2,
        out_specs=[hbm] * 2,
        scratch_shapes=[dma((3, m - 1)), dma((3,)), dma((m - 1,)), dma((m - 1,)), dma((2,))],
        compiler_params=pltpu.CompilerParams(
            collective_id=1, has_side_effects=True, vmem_limit_bytes=8 * 2**20),
        cost_estimate=pl.CostEstimate(
            flops=2 * n * rows * total * rank, bytes_accessed=n * rows * total, transcendentals=0),
    )(part, normz)

    tile = 128 if rows % 128 == 0 else rows
    halves = 2 if min(cq, ck, cv) % 256 == 0 and ck == cv and cq % ck == 0 else 1
    starts = (0, cq, cq + ck)
    widths = (cq // halves, ck // halves, cv // halves)

    def block(width):
        return pl.BlockSpec((1, rows, width), lambda j, i: (i, 0, j))

    def placed(width):
        return pl.BlockSpec((rows, width), lambda j, i: (i, j))

    def columns(height, width):
        return pl.BlockSpec((height, width), lambda j, i: (0, j))

    def scales(start, width):
        return pl.BlockSpec((1, width), lambda j, i: (0, start // width + j))

    before_q, before_k, before_v, col_q, col_k, col_v = pl.pallas_call(
        functools.partial(merge_kernel, tile),
        grid=(halves, n),
        out_shape=[jax.ShapeDtypeStruct((n * rows, c), BF16) for c in (cq, ck, cv)]
        + [jax.ShapeDtypeStruct((1, c), F32) for c in (cq, ck, cv)],
        in_specs=[block(c) for c in widths]
        + [pl.BlockSpec((3, 1, rank, rows), lambda j, i: (0, i, 0, 0))]
        + [columns(rank, c) for c in widths]
        + [scales(start, c) for start, c in zip(starts, widths)],
        out_specs=[placed(c) for c in widths] + [columns(1, c) for c in widths],
        compiler_params=pltpu.CompilerParams(vmem_limit_bytes=60 * 2**20),
        cost_estimate=pl.CostEstimate(
            flops=2 * n * rows * total * rank, bytes_accessed=4 * n * rows * total, transcendentals=0),
    )(gq, gk, gv, glow, hq, hk, hv, col, col, col)

    def finish(i, came, tail, high, before, first, wanted):
        size, width = came.shape
        step = 128 if size % 128 == 0 else size
        start = starts[i]
        return pl.pallas_call(
            functools.partial(last_kernel, n, first, step, wanted),
            grid=(1,),
            out_shape=jax.ShapeDtypeStruct((n * rows, width), BF16),
            in_specs=[vmem, vmem,
                      pl.BlockSpec((1, 1, rank, rows), lambda t: (i, 0, 0, 0)),
                      pl.BlockSpec((1, 1, rank, rows), lambda t: (i, n - 1, 0, 0)),
                      vmem,
                      pl.BlockSpec((1, width), lambda t: (0, start // width)), hbm],
            out_specs=hbm,
            scratch_shapes=[pltpu.VMEM((size, width), BF16), dma((size // step,))],
            input_output_aliases={6: 0},
            compiler_params=pltpu.CompilerParams(vmem_limit_bytes=12 * 2**20),
            cost_estimate=pl.CostEstimate(
                flops=2 * size * width * rank, bytes_accessed=4 * size * width, transcendentals=0),
        )(came, tail, glow, glow, high, col, before)

    fq = finish(0, came_q, tail_q, hq, before_q, pieces[spare][1], trials - 1)
    fk = finish(1, came_k, tail_k, hk, before_k, 0, None)
    most = finish(2, came_v, tail_v, hv, before_v, 0, None)
    fv = finish(2, came_w, tail_w, hv, most, pieces[-1][1], None)
    return (fq, fk, fv, col_q[0], col_k[0], col_v[0], norm.reshape(-1).astype(BF16))


def solution(mesh):
    placed = (
        P(("trial", "fsdp"), "width"), P(("trial", "fsdp"), None), P("trial", "width"),
        P(("trial", "fsdp"), "width"), P(("trial", "fsdp"), None), P("trial", "width"),
        P(("trial", "fsdp"), "width"), P(("trial", "fsdp"), None), P("trial", "width"),
        P(("trial", "fsdp", "width")), P(("trial", "fsdp", "width")),
    )
    return jax.shard_map(
        functools.partial(local, mesh.shape["fsdp"], mesh.shape["width"], mesh.shape["trial"]),
        mesh=mesh,
        in_specs=placed,
        out_specs=(
            P("trial", "width"), P("trial", "width"), P("trial", "width"),
            P(("trial", "width")), P(("trial", "width")), P(("trial", "width")),
            P("trial"),
        ),
        check_vma=False,
    )
```

```python
import functools

import jax
import jax.numpy as jnp
from jax import lax
from jax.experimental import pallas as pl
from jax.experimental.pallas import tpu as pltpu
from jax.sharding import PartitionSpec as P


mix_rate = 2.0
MESH = pl.DeviceIdType.MESH
F32, BF16 = jnp.float32, jnp.bfloat16
WAYS = (True, False)


def pieces_of(rows, widths):
    smallest = min(widths)
    unit = 128 if rows % 128 == 0 else 8
    units = rows // unit
    pieces = []
    for a, width in enumerate(widths):
        count = min(2 * (width // smallest), units)
        cuts = [i * units // count for i in range(count + 1)]
        if a == 2:
            end = units - max(1, units // 7)
            cuts = sorted({0, (end + 1) // 2, end, units})
        pieces += [(a, unit * first, unit * (last - first)) for first, last in zip(cuts, cuts[1:])]
    return pieces


def held_of(pieces):
    return max(c for c, (a, _, _) in enumerate(pieces) if a == 0)


def carrier(i, m):
    return (m - 1 - i) % m


def line_kernel(n, m, trials, wq, wk, wv, lq, lk, lv, hq, hk, hv, nt, ns,
                gq, gk, gv, tail_q, tail_k, tail_v, tail_w, glow, col_out, norm_out,
                low_q, low_k, low_v, high_q, high_k, high_v, train, step_v, col_ref, norm_ref,
                small_sem, result_sem,
                own_q, own_k, own_v, came, leaving, vec_own,
                send_up, send_dn, recv_up, recv_dn,
                low_send, low_recv, vec_send, vec_recv,
                in_sem, out_sem, low_sem, inner):
    z, x = lax.axis_index("fsdp"), lax.axis_index("width")
    weights, gathered, owns = (wq, wk, wv), (gq, gk, gv), (own_q, own_k, own_v)
    late = lax.axis_index("trial") == trials - 1
    lows, near_lows, near_highs = (lq, lk, lv), (low_q, low_k, low_v), (high_q, high_k, high_v)
    rows = wq.shape[0]
    share = train.shape[1]
    pieces = pieces_of(rows, [w.shape[1] for w in weights])
    count = len(pieces)
    spare = held_of(pieces)

    def aside_of(c):
        a, first, size = pieces[c]
        if c == spare or c == count - 1:
            return (tail_q if c == spare else tail_w).at[pl.ds(0, size)]
        return (tail_k if a == 1 else tail_v).at[pl.ds(first, size)]

    loads = [pltpu.make_async_copy(w, o, in_sem.at[i]) for i, (w, o) in enumerate(zip(weights, owns))]
    smalls = [
        pltpu.make_async_copy(a, b, small_sem.at[i])
        for i, (a, b) in enumerate(zip(lows + (hq, hk, hv, nt, ns), near_lows + near_highs + (train, step_v)))
    ]

    barrier = pltpu.get_barrier_semaphore()
    middle = n // 2

    def tell(semaphore, when, upward):
        @pl.when(when)
        def _():
            pl.semaphore_signal(semaphore, inc=1, device_id_type=MESH, device_id={
                "fsdp": jnp.minimum(z + 1, n - 1) if upward else jnp.maximum(z - 1, 0)})

    tell(barrier, z < middle, True)
    tell(barrier, z > middle, False)

    def sent_block(hop, up):
        return jnp.clip(z - (hop - 1) if up else z + (hop - 1), 0, n - 1)

    def next_on(up):
        return jnp.clip(z + 1 if up else z - 1, 0, n - 1)

    def sends(hop, up):
        return (z >= hop - 1) & (z < n - 1) if up else (z + hop - 1 <= n - 1) & (z > 0)

    def receives(hop, up):
        return z >= hop if up else z + hop <= n - 1

    def held(c):
        return late if c == spare else pieces[c][0] > 0

    def travels(hop, c, when):
        if hop < n - 1 or held(c) is False:
            return when
        return False if held(c) is True else when & jnp.logical_not(held(c))

    def piece(hop, c, up, aside=False):
        a, first, size = pieces[c]
        block = sent_block(hop, up)
        landing = gathered[a].at[block, pl.ds(first, size)]
        source = weights[a].at[pl.ds(first, size)] if hop == 1 else landing
        if aside:
            landing = aside_of(c)
        out, back = (send_up, recv_up) if up else (send_dn, recv_dn)
        return pltpu.make_async_remote_copy(
            src_ref=source, dst_ref=landing,
            send_sem=out.at[hop - 1, c], recv_sem=back.at[hop - 1, c],
            device_id={"fsdp": next_on(up)}, device_id_type=MESH,
        )

    def start_piece(hop, c, up):
        when = travels(hop, c, sends(hop, up))
        if when is False:
            return
        if hop == n - 2 and held(c) is not False:
            aside = (z == n - 3) if up else (z == 2)
            if held(c) is not True:
                aside = aside & held(c)

            @pl.when(when & aside)
            def _():
                piece(hop, c, up, True).start()

            @pl.when(when & jnp.logical_not(aside))
            def _():
                piece(hop, c, up).start()
        else:
            @pl.when(when)
            def _():
                piece(hop, c, up).start()

    def low_piece(hop, i, up):
        block = sent_block(hop, up)
        return pltpu.make_async_remote_copy(
            src_ref=lows[i] if hop == 1 else glow.at[block], dst_ref=glow.at[block],
            send_sem=low_send.at[int(up), hop - 1], recv_sem=low_recv.at[int(up), hop - 1],
            device_id={"fsdp": next_on(up)}, device_id_type=MESH)

    def message(up, first=False):
        return pltpu.make_async_remote_copy(
            src_ref=vec_own if first else leaving.at[int(up)], dst_ref=came.at[int(up)],
            send_sem=vec_send.at[int(up)], recv_sem=vec_recv.at[int(up)],
            device_id={"fsdp": next_on(up)}, device_id_type=MESH)

    def carried(i):
        return x == carrier(i, m)

    @pl.when((z > 0) & (z < n - 1) & (z != middle))
    def _():
        pl.semaphore_wait(barrier, 1)

    @pl.when(z == middle)
    def _():
        pl.semaphore_wait(barrier, 2 if middle < n - 1 else 1)

    def start_low(up):
        for i in range(3):
            @pl.when(carried(i) & sends(1, up))
            def _(i=i):
                low_piece(1, i, up).start()

    lead = min(3, count)

    def start_lead(up):
        for c in range(lead):
            start_piece(1, c, up)
        start_low(up)

    @pl.when(z >= middle)
    def _():
        start_lead(True)

    @pl.when(z <= middle)
    def _():
        start_lead(False)

    tell(inner, (z > 0) & (z <= middle), False)
    tell(inner, (z >= middle) & (z < n - 1), True)

    @pl.when(z != middle)
    def _():
        pl.semaphore_wait(inner, 1)

    @pl.when(z < middle)
    def _():
        start_lead(True)

    @pl.when(z > middle)
    def _():
        start_lead(False)

    for copy in loads + smalls:
        copy.start()
    for small in smalls:
        small.wait()
    for i in range(3):
        @pl.when(carried(i))
        def _(i=i):
            pltpu.make_async_copy(near_lows[i], glow.at[z], low_sem).start()
    for load in loads:
        load.wait()
    stores = [pltpu.make_async_copy(o, g.at[z], out_sem.at[i]) for i, (g, o) in enumerate(zip(gathered, owns))]
    for store in stores:
        store.start()
    total = col_ref.shape[1]
    slot = (vec_own.shape[1] - total) // n
    vec_own[...] = jnp.zeros_like(vec_own)
    tile = 128 if rows % 128 == 0 else rows
    at = 0
    for low, high, own in zip(near_lows, near_highs, owns):
        width = own.shape[1]

        def step(i, best, low=low, high=high, own=own):
            span = pl.ds(pl.multiple_of(i * tile, tile), tile)
            delta = lax.dot_general(
                low[:, span], high[...], (((0,), (0,)), ((), ())), preferred_element_type=F32)
            result = own[span, :].astype(F32) + mix_rate * delta
            return jnp.maximum(best, jnp.max(jnp.abs(result), axis=0, keepdims=True))

        vec_own[:, pl.ds(at, width)] = lax.fori_loop(0, rows // tile, step, jnp.zeros((1, width), F32))
        at += width
    gain = train[...] + step_v[...]
    for b in range(n):
        vec_own[:, pl.ds(total + b * slot, share)] = jnp.where(z == b, gain, 0.0)

    @pl.when(z == 0)
    def _():
        message(True, True).start()

    @pl.when(z == n - 1)
    def _():
        message(False, True).start()

    for c in range(lead, count):
        for up in (False, True):
            start_piece(1, c, up)

    results = [pltpu.make_async_copy(col_ref, col_out, result_sem.at[0]),
               pltpu.make_async_copy(norm_ref, norm_out, result_sem.at[1])]

    def join(mine, other):
        peak = jnp.maximum(mine[:, :total], other[:, :total])
        return jnp.concatenate([peak, mine[:, total:] + other[:, total:]], axis=1)

    def small_turn(hop):
        for up in WAYS:
            @pl.when((z == hop) if up else (z == n - 1 - hop))
            def _(up=up):
                message(up).wait_recv()

                @pl.when((z < n - 1) if up else (z > 0))
                def _():
                    leaving[int(up)] = join(vec_own[...], came[int(up)])
                    message(up).start()

            @pl.when(receives(hop, up))
            def _(up=up):
                for i in range(3):
                    @pl.when(carried(i))
                    def _(i=i):
                        low_piece(hop, i, up).wait_recv()
                        if hop < n - 1:
                            @pl.when(sends(hop + 1, up))
                            def _():
                                low_piece(hop + 1, i, up).start()
        if hop == n - 1:
            col_ref[...] = vec_own[:, pl.ds(0, total)]
            for b in range(n):
                norm_ref[b] = vec_own[:, pl.ds(total + b * slot, share)]
            for up in WAYS:
                @pl.when((z > 0) if up else (z < n - 1))
                def _(up=up):
                    col_ref[...] = jnp.maximum(col_ref[...], came[int(up), :, pl.ds(0, total)])
                    for b in range(n):
                        norm_ref[b] += came[int(up), :, pl.ds(total + b * slot, share)]
            for result in results:
                result.start()

    turn = min(1, spare)
    for hop in range(1, n):
        for c in range(count):
            if held(c) is True and hop == n - 1:
                continue
            for up in WAYS:
                @pl.when(travels(hop, c, receives(hop, up)))
                def _(hop=hop, c=c, up=up):
                    piece(hop, c, up).wait_recv()

                if hop < n - 1:
                    start_piece(hop + 1, c, up)
            if c == turn:
                small_turn(hop)
    for copy in stores + results:
        copy.wait()

    @pl.when(z < n - 1)
    def _():
        message(True).wait_send()

    @pl.when(z > 0)
    def _():
        message(False).wait_send()

    for i in range(3):
        @pl.when(carried(i))
        def _(i=i):
            pltpu.make_async_copy(near_lows[i], glow.at[z], low_sem).wait()
    for hop in range(1, n):
        for up in WAYS:
            @pl.when(sends(hop, up))
            def _(hop=hop, up=up):
                for i in range(3):
                    @pl.when(carried(i))
                    def _(i=i):
                        low_piece(hop, i, up).wait_send()

            for c in range(count):
                if held(c) is True and hop == n - 1:
                    continue

                @pl.when(travels(hop, c, sends(hop, up)))
                def _(hop=hop, c=c, up=up):
                    piece(hop, c, up).wait_send()


def plane_kernel(m, low_ref, norm_ref, glow, norm, low_send, low_recv, norm_send, norm_recv, own_sem):
    x = lax.axis_index("width")
    barrier = pltpu.get_barrier_semaphore()
    for d in range(1, m):
        pl.semaphore_signal(barrier, inc=1, device_id_type=MESH, device_id={"width": lax.rem(x + d, m)})
    own = pltpu.make_async_copy(norm_ref, norm.at[:, x], own_sem.at[1])
    own.start()
    pl.semaphore_wait(barrier, m - 1)

    def low_to(i, d):
        return pltpu.make_async_remote_copy(
            src_ref=low_ref, dst_ref=glow.at[i], send_sem=low_send.at[i, d - 1], recv_sem=low_recv.at[i],
            device_id={"width": lax.rem(x + d, m)}, device_id_type=MESH)

    def norm_to(d):
        return pltpu.make_async_remote_copy(
            src_ref=norm_ref, dst_ref=norm.at[:, x], send_sem=norm_send.at[d - 1], recv_sem=norm_recv.at[d - 1],
            device_id={"width": lax.rem(x + d, m)}, device_id_type=MESH)

    for i in range(3):
        @pl.when(x == carrier(i, m))
        def _(i=i):
            for d in range(1, m):
                low_to(i, d).start()
            pltpu.make_async_copy(low_ref, glow.at[i], own_sem.at[0]).start()
    for d in range(1, m):
        norm_to(d).start()
    own.wait()
    for d in range(1, m):
        norm_to(d).wait()
    for i in range(3):
        @pl.when(x == carrier(i, m))
        def _(i=i):
            pltpu.make_async_copy(low_ref, glow.at[i], own_sem.at[0]).wait()
            for d in range(1, m):
                low_to(i, d).wait_send()

        @pl.when(x != carrier(i, m))
        def _(i=i):
            low_to(i, 1).wait_recv()


def merged(weight, low, high, scale):
    delta = lax.dot_general(low, high, (((0,), (0,)), ((), ())), preferred_element_type=F32)
    return ((weight.astype(F32) + mix_rate * delta) * scale).astype(BF16)


def merge_kernel(tile, gq, gk, gv, glow, hq, hk, hv, col_q, col_k, col_v, fq, fk, fv, cq, ck, cv):
    arrays = ((gq, hq, col_q, fq), (gk, hk, col_k, fk), (gv, hv, col_v, fv))
    for col, c in ((col_q, cq), (col_k, ck), (col_v, cv)):
        c[...] = col[...]

    def step(t, carry):
        span = pl.ds(pl.multiple_of(t * tile, tile), tile)
        for i, (g, high, col, f) in enumerate(arrays):
            f[span, :] = merged(g[0, span, :], glow[i, 0, :, span], high[...], 1.0 / col[...])
        return carry

    lax.fori_loop(0, gq.shape[1] // tile, step, 0)


def last_kernel(n, first, tile, wanted, came, tail, low_first, low_last, high, col, before, final, out_ref, out_sem):
    z = lax.axis_index("fsdp")
    size = came.shape[0]
    rows = low_first.shape[3]

    def store(p, block):
        return pltpu.make_async_copy(
            out_ref.at[pl.ds(p * tile, tile)],
            final.at[pl.ds(block * rows + first + p * tile, tile)], out_sem.at[p])

    def write(source, low, block):
        scale = 1.0 / col[...]
        for p in range(size // tile):
            span = pl.ds(p * tile, tile)
            out_ref[span, :] = merged(source[span, :], low[0, 0, :, pl.ds(first + p * tile, tile)], high[...], scale)
            store(p, block).start()
        for p in range(size // tile):
            store(p, block).wait()

    for at, source, low, block in ((0, came, low_last, n - 1), (1, tail, low_last, n - 1),
                                   (n - 2, tail, low_first, 0), (n - 1, came, low_first, 0)):
        here = z == at
        if wanted is not None:
            here = here & (lax.axis_index("trial") == wanted)

        @pl.when(here)
        def _(source=source, low=low, block=block):
            write(source, low, block)


def ready_kernel(first, low_first, low_last, high, col, plus, scale):
    z = lax.axis_index("fsdp")
    size = plus.shape[0]
    scale[...] = 1.0 / col[...]

    def fill(low):
        plus[...] = mix_rate * lax.dot_general(
            low[0, 0, :, pl.ds(first, size)], high[...], (((0,), (0,)), ((), ())), preferred_element_type=F32)

    @pl.when(z < 2)
    def _():
        fill(low_last)

    @pl.when(z >= 2)
    def _():
        fill(low_first)


def close_kernel(n, first, came, tail, plus, scale, before, final, out_ref, out_sem):
    z = lax.axis_index("fsdp")
    size = came.shape[0]
    rows = final.shape[0] // n

    for at, source, block in ((0, came, n - 1), (1, tail, n - 1), (n - 2, tail, 0), (n - 1, came, 0)):
        @pl.when(z == at)
        def _(source=source, block=block):
            out_ref[...] = ((source[...].astype(F32) + plus[...]) * scale[...]).astype(BF16)
            store = pltpu.make_async_copy(out_ref, final.at[pl.ds(block * rows + first, size)], out_sem)
            store.start()
            store.wait()


def local(n, m, trials, wq, lq, hq, wk, lk, hk, wv, lv, hv, nt, ns):
    rows, cq = wq.shape
    ck, cv = wk.shape[1], wv.shape[1]
    rank, share = hq.shape[0], nt.shape[0]
    total = cq + ck + cv
    length = total + n * (-(-share // 128) * 128)
    pieces = pieces_of(rows, [cq, ck, cv])
    count, spare = len(pieces), held_of(pieces)
    hbm, vmem = pl.BlockSpec(memory_space=pl.ANY), pl.BlockSpec(memory_space=pltpu.VMEM)
    dma = pltpu.SemaphoreType.DMA
    gq, gk, gv, tail_q, tail_k, tail_v, tail_w, part, col, normz = pl.pallas_call(
        functools.partial(line_kernel, n, m, trials),
        out_shape=[
            jax.ShapeDtypeStruct((n, rows, cq), BF16),
            jax.ShapeDtypeStruct((n, rows, ck), BF16),
            jax.ShapeDtypeStruct((n, rows, cv), BF16),
            jax.ShapeDtypeStruct((pieces[spare][2], cq), BF16),
            jax.ShapeDtypeStruct((rows, ck), BF16),
            jax.ShapeDtypeStruct((rows - pieces[-1][2], cv), BF16),
            jax.ShapeDtypeStruct((pieces[-1][2], cv), BF16),
            jax.ShapeDtypeStruct((n, rank, rows), BF16),
            jax.ShapeDtypeStruct((1, total), F32),
            jax.ShapeDtypeStruct((n, 1, share), F32),
        ],
        in_specs=[hbm] * 11,
        out_specs=[hbm] * 10,
        scratch_shapes=[
            pltpu.VMEM((rank, rows), BF16), pltpu.VMEM((rank, rows), BF16), pltpu.VMEM((rank, rows), BF16),
            pltpu.VMEM((rank, cq), BF16), pltpu.VMEM((rank, ck), BF16), pltpu.VMEM((rank, cv), BF16),
            pltpu.VMEM((1, share), F32), pltpu.VMEM((1, share), F32),
            pltpu.VMEM((1, total), F32), pltpu.VMEM((n, 1, share), F32), dma((8,)), dma((2,)),
            pltpu.VMEM((rows, cq), BF16), pltpu.VMEM((rows, ck), BF16), pltpu.VMEM((rows, cv), BF16),
            pltpu.VMEM((2, 1, length), F32), pltpu.VMEM((2, 1, length), F32), pltpu.VMEM((1, length), F32),
            dma((n - 1, count)), dma((n - 1, count)), dma((n - 1, count)), dma((n - 1, count)),
            dma((2, n - 1)), dma((2, n - 1)), dma((2,)), dma((2,)),
            dma((3,)), dma((3,)), dma, pltpu.SemaphoreType.REGULAR,
        ],
        compiler_params=pltpu.CompilerParams(collective_id=0, has_side_effects=True),
    )(wq, wk, wv, lq.T, lk.T, lv.T, hq, hk, hv, nt.reshape(1, share), ns.reshape(1, share))

    ends = [(1, 0), (n - 2, n - 1)]
    lone = [(a * trials + trials - 1, b * trials + trials - 1) for a, b in ends]
    came_q = lax.ppermute(tail_q, ("fsdp", "trial"), lone)
    came_k = lax.ppermute(tail_k, "fsdp", ends)
    came_v = lax.ppermute(tail_v, "fsdp", ends)
    came_w = lax.ppermute(tail_w, "fsdp", ends)

    glow, norm = pl.pallas_call(
        functools.partial(plane_kernel, m),
        out_shape=[
            jax.ShapeDtypeStruct((3, n, rank, rows), BF16),
            jax.ShapeDtypeStruct((n, m, 1, share), F32),
        ],
        in_specs=[vmem] * 2,
        out_specs=[hbm] * 2,
        scratch_shapes=[dma((3, m - 1)), dma((3,)), dma((m - 1,)), dma((m - 1,)), dma((2,))],
        compiler_params=pltpu.CompilerParams(
            collective_id=1, has_side_effects=True, vmem_limit_bytes=8 * 2**20),
        cost_estimate=pl.CostEstimate(
            flops=2 * n * rows * total * rank, bytes_accessed=n * rows * total, transcendentals=0),
    )(part, normz)

    tile = 128 if rows % 128 == 0 else rows
    halves = 2 if min(cq, ck, cv) % 256 == 0 and ck == cv and cq % ck == 0 else 1
    starts = (0, cq, cq + ck)
    widths = (cq // halves, ck // halves, cv // halves)

    def block(width):
        return pl.BlockSpec((1, rows, width), lambda j, i: (i, 0, j))

    def placed(width):
        return pl.BlockSpec((rows, width), lambda j, i: (i, j))

    def columns(height, width):
        return pl.BlockSpec((height, width), lambda j, i: (0, j))

    def scales(start, width):
        return pl.BlockSpec((1, width), lambda j, i: (0, start // width + j))

    before_q, before_k, before_v, col_q, col_k, col_v = pl.pallas_call(
        functools.partial(merge_kernel, tile),
        grid=(halves, n),
        out_shape=[jax.ShapeDtypeStruct((n * rows, c), BF16) for c in (cq, ck, cv)]
        + [jax.ShapeDtypeStruct((1, c), F32) for c in (cq, ck, cv)],
        in_specs=[block(c) for c in widths]
        + [pl.BlockSpec((3, 1, rank, rows), lambda j, i: (0, i, 0, 0))]
        + [columns(rank, c) for c in widths]
        + [scales(start, c) for start, c in zip(starts, widths)],
        out_specs=[placed(c) for c in widths] + [columns(1, c) for c in widths],
        compiler_params=pltpu.CompilerParams(vmem_limit_bytes=60 * 2**20),
        cost_estimate=pl.CostEstimate(
            flops=2 * n * rows * total * rank, bytes_accessed=4 * n * rows * total, transcendentals=0),
    )(gq, gk, gv, glow, hq, hk, hv, col, col, col)

    def finish(i, came, tail, high, before, first, wanted):
        size, width = came.shape
        step = 128 if size % 128 == 0 else size
        start = starts[i]
        return pl.pallas_call(
            functools.partial(last_kernel, n, first, step, wanted),
            grid=(1,),
            out_shape=jax.ShapeDtypeStruct((n * rows, width), BF16),
            in_specs=[vmem, vmem,
                      pl.BlockSpec((1, 1, rank, rows), lambda t: (i, 0, 0, 0)),
                      pl.BlockSpec((1, 1, rank, rows), lambda t: (i, n - 1, 0, 0)),
                      vmem,
                      pl.BlockSpec((1, width), lambda t: (0, start // width)), hbm],
            out_specs=hbm,
            scratch_shapes=[pltpu.VMEM((size, width), BF16), dma((size // step,))],
            input_output_aliases={6: 0},
            compiler_params=pltpu.CompilerParams(vmem_limit_bytes=12 * 2**20),
            cost_estimate=pl.CostEstimate(
                flops=2 * size * width * rank, bytes_accessed=4 * size * width, transcendentals=0),
        )(came, tail, glow, glow, high, col, before)

    fq = finish(0, came_q, tail_q, hq, before_q, pieces[spare][1], trials - 1)
    fk = finish(1, came_k, tail_k, hk, before_k, 0, None)
    most = finish(2, came_v, tail_v, hv, before_v, 0, None)
    first, size = pieces[-1][1], pieces[-1][2]
    plus, scale = pl.pallas_call(
        functools.partial(ready_kernel, first),
        grid=(1,),
        out_shape=[jax.ShapeDtypeStruct((size, cv), F32), jax.ShapeDtypeStruct((1, cv), F32)],
        in_specs=[pl.BlockSpec((1, 1, rank, rows), lambda t: (2, 0, 0, 0)),
                  pl.BlockSpec((1, 1, rank, rows), lambda t: (2, n - 1, 0, 0)),
                  vmem, pl.BlockSpec((1, cv), lambda t: (0, starts[2] // cv))],
        out_specs=[vmem] * 2,
        compiler_params=pltpu.CompilerParams(vmem_limit_bytes=12 * 2**20),
        cost_estimate=pl.CostEstimate(
            flops=2 * size * cv * rank, bytes_accessed=4 * size * cv, transcendentals=0),
    )(glow, glow, hv, col)
    fv = pl.pallas_call(
        functools.partial(close_kernel, n, first),
        out_shape=jax.ShapeDtypeStruct((n * rows, cv), BF16),
        in_specs=[vmem] * 4 + [hbm],
        out_specs=hbm,
        scratch_shapes=[pltpu.VMEM((size, cv), BF16), dma],
        input_output_aliases={4: 0},
        compiler_params=pltpu.CompilerParams(vmem_limit_bytes=12 * 2**20),
        cost_estimate=pl.CostEstimate(
            flops=2 * size * cv, bytes_accessed=4 * size * cv, transcendentals=0),
    )(came_w, tail_w, plus, scale, most)
    return (fq, fk, fv, col_q[0], col_k[0], col_v[0], norm.reshape(-1).astype(BF16))


def solution(mesh):
    placed = (
        P(("trial", "fsdp"), "width"), P(("trial", "fsdp"), None), P("trial", "width"),
        P(("trial", "fsdp"), "width"), P(("trial", "fsdp"), None), P("trial", "width"),
        P(("trial", "fsdp"), "width"), P(("trial", "fsdp"), None), P("trial", "width"),
        P(("trial", "fsdp", "width")), P(("trial", "fsdp", "width")),
    )
    return jax.shard_map(
        functools.partial(local, mesh.shape["fsdp"], mesh.shape["width"], mesh.shape["trial"]),
        mesh=mesh,
        in_specs=placed,
        out_specs=(
            P("trial", "width"), P("trial", "width"), P("trial", "width"),
            P(("trial", "width")), P(("trial", "width")), P(("trial", "width")),
            P("trial"),
        ),
        check_vma=False,
    )
```
